128 devices in a mesh: gx: 4 (over x), gy: 4 (over z_lo, core), gz: 8 (over z_hi, y).
Axes of the slice: x: 4, y: 4, z: 4 (z_hi: 2, z_lo: 2; z = z_hi * 2 + z_lo), core: 2. Of those that a mesh axis runs over, the one named last changes fastest.
Arguments:
- orbitals: float32 [16, 48, 48, 1024], P(None, 'gx', 'gy', 'gz'), may hold values from -6 to 6
- potential: float32 [48, 48, 1024], P('gx', 'gy', 'gz'), may hold values from 0 to 2
Outputs:
- filtered: float32 [16, 48, 48, 1024], P(None, 'gx', 'gy', 'gz')
The draws below stay inside these ranges and needn't reach their ends.
All inputs are finite; a program needn't handle non-finite values.
Results may differ from the reference program's by a relative error of at most 0.00002.
Values sent between devices are 32-bit elements; how exact they have to be, the bound alone decides.
A program may use at most 64 MiB of HBM per device.

```python
import jax
import jax.numpy as jnp
from jax import lax

BANDS = 16
DEGREE = 2
NX = 48
NY = 48
NZ = 1024


def level_of(key, dims, cuts, least, high):
    loudness = 1.0
    for axis_at, blocks in cuts:
        heights = jax.random.uniform(jax.random.fold_in(jax.random.fold_in(key, 6), axis_at), (blocks,), jnp.float32, least / len(cuts), high / len(cuts))
        loudness = loudness * jnp.repeat(jnp.exp(heights), dims[axis_at] // blocks).reshape((-1,) + (1,) * (len(dims) - 1 - axis_at))
    return loudness


def normal_values(stream_key, dims, scale, most, split=(), kind=jnp.bfloat16):
    level = level_of(stream_key, dims, split, -0.22, 0.18) if split else 1.0
    array = jax.random.normal(stream_key, dims, jnp.float32) * scale * level
    return jnp.minimum(jnp.maximum(array, -most), most).astype(kind)


def setup_inputs(seed: int = 0) -> dict:
    streams_of = jax.random.split(jax.random.key(seed), 3)
    return {
        "orbitals": normal_values(streams_of[0], (BANDS, NX, NY, NZ), 1.0, 6.0, ((1, 4), (2, 4), (3, 8)), jnp.float32),
        "potential": jnp.clip(2.0 * jax.random.uniform(streams_of[1], (NX, NY, NZ), jnp.float32) ** level_of(streams_of[1], (NX, NY, NZ), ((0, 4), (1, 4), (2, 8)), -0.2, 0.2), 0.0, 2.0),
    }


SECOND = (-5369.0 / 1800.0, 12.0 / 7.0, -15.0 / 56.0, 10.0 / 189.0, -1.0 / 112.0, 2.0 / 1925.0, -1.0 / 16632.0)
FIRST = (6.0 / 7.0, -15.0 / 56.0, 5.0 / 63.0, -1.0 / 56.0, 3.0 / 385.0, -1.0 / 792.0)
METRIC = ((1.0, 0.25, 0.15), (0.25, 1.0, 0.2), (0.15, 0.2, 1.0))
CENTER = 10.5
HALF_WIDTH = 9.5


def window(values, starts, lengths):
    leading = values.ndim - 3
    starts_full = (0,) * leading + tuple(starts)
    limits = tuple(values.shape[:leading]) + tuple(s + l for s, l in zip(starts, lengths))
    return lax.slice(values, starts_full, limits)


def apply_operator(padded, potential):
    lengths = [padded.shape[i + 1] - 12 for i in range(3)]
    centre = window(padded, (6, 6, 6), lengths)
    summed = METRIC[0][0] * 0.0 * centre
    for d in range(3):
        second = SECOND[0] * centre
        for k in range(1, 7):
            forward = [6, 6, 6]
            forward[d] += k
            backward = [6, 6, 6]
            backward[d] -= k
            second = second + SECOND[k] * (window(padded, forward, lengths) + window(padded, backward, lengths))
        summed = summed + METRIC[d][d] * second
    for d, e in ((0, 1), (0, 2), (1, 2)):
        widened = list(lengths)
        widened[d] += 12
        partial_sum = None
        for k in range(1, 7):
            forward = [6, 6, 6]
            forward[d] = 0
            forward[e] += k
            backward = [6, 6, 6]
            backward[d] = 0
            backward[e] -= k
            term = FIRST[k - 1] * (window(padded, forward, widened) - window(padded, backward, widened))
            partial_sum = term if partial_sum is None else partial_sum + term
        crossed = None
        for k in range(1, 7):
            forward = [0, 0, 0]
            forward[d] = 6 + k
            backward = [0, 0, 0]
            backward[d] = 6 - k
            term = FIRST[k - 1] * (window(partial_sum, forward, lengths) - window(partial_sum, backward, lengths))
            crossed = term if crossed is None else crossed + term
        summed = summed + 2.0 * METRIC[d][e] * crossed
    return -0.5 * summed + potential[None] * centre


def reference(orbitals, potential):
    previous = jnp.zeros_like(orbitals)
    current = orbitals
    for degree_step in range(DEGREE):
        padded = jnp.pad(current, ((0, 0), (6, 6), (6, 6), (6, 6)), mode="wrap")
        applied = apply_operator(padded, potential)
        factor = 1.0 if degree_step == 0 else 2.0
        carry_factor = 0.0 if degree_step == 0 else 1.0
        following = factor * (applied - CENTER * current) / HALF_WIDTH - carry_factor * previous
        previous = current
        current = following
    return current
```

```python
import functools

import jax
import jax.numpy as jnp
import numpy as np
from jax import lax
from jax.experimental import pallas as pl
from jax.experimental.pallas import tpu as pltpu
from jax.sharding import PartitionSpec as P

MESH = pl.DeviceIdType.MESH
SECOND = (
    -5369.0 / 1800.0,
    12.0 / 7.0,
    -15.0 / 56.0,
    10.0 / 189.0,
    -1.0 / 112.0,
    2.0 / 1925.0,
    -1.0 / 16632.0,
)
FIRST = (6.0 / 7.0, -15.0 / 56.0, 5.0 / 63.0, -1.0 / 56.0, 3.0 / 385.0, -1.0 / 792.0)
G01, G02, G12 = 0.25, 0.15, 0.2
CENTER = 10.5
HALF_WIDTH = 9.5
SIGMA = -0.5 / HALF_WIDTH

XC = [SIGMA * c for c in SECOND]
XA = [SIGMA * 2.0 * G02 * a for a in FIRST]

F32 = jnp.float32
BF16 = jnp.bfloat16
STRIDE = 16
ROWS = 12 * STRIDE


def order_of_rows():
    rows = []
    for s in range(4):
        rows += [12 * s + r for r in range(8)]
    for s in range(4):
        rows += [12 * s + 8 + r for r in range(4)]
    return rows


def two_parts(m):
    hi = m.astype(np.float32).astype(jnp.bfloat16)
    lo = (m - hi.astype(np.float64)).astype(np.float32).astype(jnp.bfloat16)
    return hi, lo


def z_matrices():
    m = np.zeros((140, 256))
    for z in range(128):
        for k in range(1, 7):
            m[z + 6 + k, z] += FIRST[k - 1]
            m[z + 6 - k, z] -= FIRST[k - 1]
            m[z + 6 + k, 128 + z] += SIGMA * SECOND[k]
            m[z + 6 - k, 128 + z] += SIGMA * SECOND[k]
    inside = m[6:134]
    halo = np.zeros((128, 256))
    halo[122:128] = m[0:6]
    halo[0:6] = m[134:140]
    i1, i2 = two_parts(inside)
    h1, h2 = two_parts(halo)
    return np.stack([np.concatenate([i1, i1]), np.concatenate([i2, h1]), np.concatenate([h2, h1])])


def y_matrices():
    rows = order_of_rows()
    place = {y: r for r, y in enumerate(rows)}
    d1 = np.zeros((48, 48))
    d2 = np.zeros((48, 48))
    for y in range(48):
        for k in range(1, 7):
            d1[place[y], place[(y + k) % 48]] += FIRST[k - 1]
            d1[place[y], place[(y - k) % 48]] -= FIRST[k - 1]
            d2[place[y], place[(y + k) % 48]] += SECOND[k]
            d2[place[y], place[(y - k) % 48]] += SECOND[k]
    a1, a2 = two_parts(np.concatenate([(G01 / G02) * d1, SIGMA * d2]))
    b1, b2 = two_parts(SIGMA * 2.0 * G12 * d1)
    return np.concatenate([a1, a1, a2], axis=1), np.concatenate([b1, b1, b2], axis=1)


def split(value):
    hi = value.astype(BF16)
    lo = (value - hi.astype(F32)).astype(BF16)
    return hi, lo


def kernel(
    orb,
    pot,
    mz,
    my1,
    my2,
    out,
    sm,
    sr,
    spm,
    spr,
    v,
    rr,
    vp,
    rp,
    zs,
    zr,
    cs,
    cr,
    part,
    wf,
    v1,
    v2,
    h1,
    h2,
    tz,
    yf,
    ro,
    om,
    orr,
    tin_s,
    tin_r,
    zx_s,
    zx_r,
    xc_s,
    xc_r,
    to_s,
    to_r,
):
    gx = lax.axis_index("gx")
    gy = lax.axis_index("gy")
    gz = lax.axis_index("gz")
    x_at = [{"gx": lax.rem(gx + 3, 4)}, {"gx": lax.rem(gx + 1, 4)}]
    z_at = [{"gz": lax.rem(gz + 7, 8)}, {"gz": lax.rem(gz + 1, 8)}]
    y_of = [lax.rem(gy + d, 4) for d in range(4)]

    def copy(src, dst, send, recv, device):
        return pltpu.make_async_remote_copy(
            src_ref=src, dst_ref=dst, send_sem=send, recv_sem=recv, device_id=device, device_id_type=MESH
        )

    barrier = pltpu.get_barrier_semaphore()
    for device in x_at + z_at + [{"gy": y_of[d]} for d in range(1, 4)]:
        pl.semaphore_signal(barrier, inc=1, device_id=device, device_id_type=MESH)

    low_half = lax.broadcasted_iota(jnp.int32, (8, 128), 0) < 4
    lane = lax.broadcasted_iota(jnp.int32, (48, 128), 1)

    def pair(a, b):
        return (
            jnp.where(low_half, a, pltpu.roll(b, 4, 0)),
            jnp.where(low_half, pltpu.roll(a, 4, 0), b),
        )

    started = []

    def start(c):
        c.start()
        started.append(c)

    def tin(c, d):
        to = {"gy": y_of[d]}
        if c == 4:
            return [
                copy(spm, vp.at[:, gy], tin_s.at[c, d, 0], tin_r.at[c, d, 0], to),
                copy(spr, rp.at[gy], tin_s.at[c, d, 1], tin_r.at[c, d, 1], to),
            ]
        return [
            copy(sm.at[c, y_of[d]], v.at[c, 0, :, gy], tin_s.at[c, d, 0], tin_r.at[c, d, 0], to),
            copy(sr.at[c, y_of[d]], rr.at[c, gy], tin_s.at[c, d, 1], tin_r.at[c, d, 1], to),
        ]

    def prepare(c):
        if c == 4:
            for x in range(12):
                spm[x] = pot[x, 0:8]
            for p in range(6):
                spr[p] = jnp.concatenate([pot[2 * p, 8:12], pot[2 * p + 1, 8:12]], axis=0)
            return

        def band(g, carry):
            b = 4 * c + g
            for x in range(12):
                sm[c, g, x] = orb[pl.ds(x * ROWS + b, 8, stride=STRIDE), :]
            for p in range(6):
                lo = orb[pl.ds(2 * p * ROWS + 8 * STRIDE + b, 4, stride=STRIDE), :]
                hi = orb[pl.ds((2 * p + 1) * ROWS + 8 * STRIDE + b, 4, stride=STRIDE), :]
                sr[c, g, p] = jnp.concatenate([lo, hi], axis=0)
            return carry

        lax.fori_loop(0, 4, band, 0)

    def keep_own(c):
        if c == 4:
            vp[:, gy] = spm[...]
            rp[gy] = spr[...]
        else:
            v[c, 0, :, gy] = sm[c, gy]
            rr[c, gy] = sr[c, gy]

    def assemble(rest, dest):
        for p in range(6):
            for t in range(2):
                even, odd = pair(rest[2 * t, p], rest[2 * t + 1, p])
                dest(2 * p, 4 + t, even)
                dest(2 * p + 1, 4 + t, odd)

    def zx(c, step, side):
        return copy(
            zs.at[c, step, side], zr.at[c, step, 1 - side], zx_s.at[c, step, side], zx_r.at[c, step, side], z_at[side]
        )

    def edges(c, step):
        low = None
        high = None
        for x in range(12):
            val = v[c, step, x].reshape(48, 128)
            a = val if x == 0 else pltpu.roll(val, 6 * x, 1)
            b = pltpu.roll(val, 6 * x + 6, 1)
            low = a if x == 0 else jnp.where(lane >= 6 * x, a, low)
            high = b if x == 0 else jnp.where(lane >= 6 * x, b, high)
        zs[c, step, 0] = low.reshape(6, 8, 128)
        zs[c, step, 1] = high.reshape(6, 8, 128)
        for side in range(2):
            start(zx(c, step, side))

    def stage_a(c):
        for d in range(1, 4):
            for one in tin(c, d):
                one.wait_recv()

        def dest(x, t, value):
            v[c, 0, x, t] = value

        assemble(rr.at[c], dest)
        edges(c, 0)

    def xc(c, step, side):
        return copy(
            cs.at[c, step, side], cr.at[c, step, side], xc_s.at[c, step, side], xc_r.at[c, step, side], x_at[side]
        )

    def stage_b(c, step):
        for x in range(12):
            a, b = split(v[c, step, x].reshape(48, 128))
            v1[x] = a
            v2[x] = b
        for side in range(2):
            zx(c, step, side).wait_recv()
        below = zr[c, step, 0].reshape(48, 128)
        above = zr[c, step, 1].reshape(48, 128)
        for x in range(12):
            up = above if x == 0 else pltpu.roll(above, 128 - 6 * x, 1)
            down = pltpu.roll(below, 122 - 6 * x, 1)
            h = jnp.where(lane < 6, up, jnp.where(lane >= 122, down, 0.0))
            a, b = split(h)
            h1[x] = a
            h2[x] = b
        f1 = v1[...].reshape(576, 128)
        f2 = v2[...].reshape(576, 128)
        g1 = h1[...].reshape(576, 128)
        g2 = h2[...].reshape(576, 128)
        acc = jnp.dot(jnp.concatenate([f1, f2], axis=1), mz[0], preferred_element_type=F32)
        acc += jnp.dot(jnp.concatenate([f1, g1], axis=1), mz[1], preferred_element_type=F32)
        acc += jnp.dot(jnp.concatenate([g1, g2], axis=1), mz[2], preferred_element_type=F32)
        tz[...] = acc
        for xp in range(6):
            x0, x1 = 2 * xp, 2 * xp + 1
            a = jnp.concatenate([v1[x0], v1[x1]], axis=1)
            b = jnp.concatenate([v2[x0], v2[x1]], axis=1)
            q = jnp.dot(my1[...], jnp.concatenate([a, b, a], axis=0), preferred_element_type=F32)
            t = jnp.concatenate([tz[48 * x0 : 48 * x0 + 48, 0:128], tz[48 * x1 : 48 * x1 + 48, 0:128]], axis=1)
            s = jnp.concatenate([tz[48 * x0 : 48 * x0 + 48, 128:256], tz[48 * x1 : 48 * x1 + 48, 128:256]], axis=1)
            ta, tb = split(t)
            r = jnp.dot(my2[...], jnp.concatenate([ta, tb, ta], axis=0), preferred_element_type=F32)
            w = q[0:48] + t
            r = r + q[48:96] + s
            for i, x in enumerate((x0, x1)):
                wf[x] = w[:, 128 * i : 128 * i + 128].reshape(6, 8, 128)
                part[c, x] = r[:, 128 * i : 128 * i + 128].reshape(6, 8, 128)

        def tile(t, carry):
            acc = [None] * 24
            for half in range(2):
                for j in range(6 * half, 6 * half + 6):
                    vj = v[c, step, j, t]
                    wj = wf[j, t]
                    for k in range(1, 7):
                        cv = XC[k] * vj
                        aw = XA[k - 1] * wj
                        lo, hi = j + 6 - k, j + 6 + k
                        acc[lo] = cv + aw if acc[lo] is None else acc[lo] + (cv + aw)
                        acc[hi] = cv - aw if acc[hi] is None else acc[hi] + (cv - aw)
            for i in range(6):
                cs[c, step, 0, i, t] = acc[i]
                cs[c, step, 1, i, t] = acc[18 + i]
            for i in range(12):
                part[c, i, t] = part[c, i, t] + acc[6 + i]
            return carry

        lax.fori_loop(0, 6, tile, 0)
        for side in range(2):
            start(xc(c, step, side))

    def to(c, d):
        at = {"gy": y_of[d]}
        return [
            copy(yf.at[c, :, y_of[d]], om.at[c, gy], to_s.at[c, d, 0], to_r.at[c, d, 0], at),
            copy(ro.at[c, y_of[d]], orr.at[c, gy], to_s.at[c, d, 1], to_r.at[c, d, 1], at),
        ]

    def stage_c(c, step):
        for side in range(2):
            xc(c, step, side).wait_recv()
        for x in range(12):
            got = cr[c, step, 1, x] if x < 6 else cr[c, step, 0, x - 6]
            y = part[c, x] + got + vp[x] * v[c, step, x]
            if step == 0:
                v[c, 1, x] = y
            else:
                yf[c, x] = 2.0 * y - v[c, 0, x]
        if step == 0:
            edges(c, 1)
            return
        for p in range(6):
            for t in range(2):
                even, odd = pair(yf[c, 2 * p, 4 + t], yf[c, 2 * p + 1, 4 + t])
                ro[c, 2 * t, p] = even
                ro[c, 2 * t + 1, p] = odd
        for d in range(1, 4):
            for one in to(c, d):
                start(one)
        om[c, gy] = yf[c, :, gy]
        orr[c, gy] = ro[c, gy]

    def stage_d(c):
        for d in range(1, 4):
            for one in to(c, d):
                one.wait_recv()

        def band(g, carry):
            b = 4 * c + g
            for x in range(12):
                out[pl.ds(x * ROWS + b, 8, stride=STRIDE), :] = om[c, g, x]
            for p in range(6):
                r = orr[c, g, p]
                out[pl.ds(2 * p * ROWS + 8 * STRIDE + b, 4, stride=STRIDE), :] = r[0:4]
                out[pl.ds((2 * p + 1) * ROWS + 8 * STRIDE + b, 4, stride=STRIDE), :] = r[4:8]
            return carry

        lax.fori_loop(0, 4, band, 0)

    def send_in(c):
        for d in (2, 1, 3):
            for one in tin(c, d):
                start(one)
        keep_own(c)

    prepare(0)
    pl.semaphore_wait(barrier, 7)
    send_in(0)
    for c in (1, 2, 4, 3):
        prepare(c)
        send_in(c)

    stage_a(0)
    stage_a(1)
    stage_b(0, 0)
    stage_a(2)
    stage_b(1, 0)
    for d in range(1, 4):
        for one in tin(4, d):
            one.wait_recv()

    def place(x, t, value):
        vp[x, t] = value

    assemble(rp, place)
    for x in range(12):
        vp[x] = (vp[x] - CENTER) * (1.0 / HALF_WIDTH) + 3.0 * XC[0]
    stage_a(3)
    stage_b(2, 0)
    stage_c(0, 0)
    stage_b(3, 0)
    stage_c(1, 0)
    stage_b(0, 1)
    stage_c(2, 0)
    stage_b(1, 1)
    stage_c(3, 0)
    stage_b(2, 1)
    stage_c(0, 1)
    stage_b(3, 1)
    stage_c(1, 1)
    stage_c(2, 1)
    stage_d(0)
    stage_c(3, 1)
    stage_d(1)
    stage_d(2)
    stage_d(3)
    for one in started:
        one.wait_send()


def local(orbitals, potential):
    rows = jnp.transpose(orbitals, (1, 2, 0, 3)).reshape(2304, 128)
    my1, my2 = y_matrices()
    vmem = pl.BlockSpec(memory_space=pltpu.VMEM)
    tile = (6, 8, 128)
    slab = (12, *tile)
    sem = pltpu.SemaphoreType.DMA
    out = pl.pallas_call(
        kernel,
        out_shape=jax.ShapeDtypeStruct((2304, 128), F32),
        in_specs=[vmem] * 5,
        out_specs=vmem,
        scratch_shapes=[
            pltpu.VMEM((4, 4, 12, 8, 128), F32),
            pltpu.VMEM((4, 4, *tile), F32),
            pltpu.VMEM((12, 8, 128), F32),
            pltpu.VMEM(tile, F32),
            pltpu.VMEM((4, 2, *slab), F32),
            pltpu.VMEM((4, 4, *tile), F32),
            pltpu.VMEM(slab, F32),
            pltpu.VMEM((4, *tile), F32),
            pltpu.VMEM((4, 2, 2, *tile), F32),
            pltpu.VMEM((4, 2, 2, *tile), F32),
            pltpu.VMEM((4, 2, 2, 6, *tile), F32),
            pltpu.VMEM((4, 2, 2, 6, *tile), F32),
            pltpu.VMEM((4, *slab), F32),
            pltpu.VMEM(slab, F32),
            pltpu.VMEM((12, 48, 128), BF16),
            pltpu.VMEM((12, 48, 128), BF16),
            pltpu.VMEM((12, 48, 128), BF16),
            pltpu.VMEM((12, 48, 128), BF16),
            pltpu.VMEM((576, 256), F32),
            pltpu.VMEM((4, *slab), F32),
            pltpu.VMEM((4, 4, *tile), F32),
            pltpu.VMEM((4, 4, 12, 8, 128), F32),
            pltpu.VMEM((4, 4, *tile), F32),
            sem((5, 4, 2)),
            sem((5, 4, 2)),
            sem((4, 2, 2)),
            sem((4, 2, 2)),
            sem((4, 2, 2)),
            sem((4, 2, 2)),
            sem((4, 4, 2)),
            sem((4, 4, 2)),
        ],
        compiler_params=pltpu.CompilerParams(
            collective_id=0, has_side_effects=True, vmem_limit_bytes=60 * 1024 * 1024
        ),
    )(rows, potential, jnp.asarray(z_matrices()), jnp.asarray(my1), jnp.asarray(my2))
    return jnp.transpose(out.reshape(12, 12, 16, 128), (2, 0, 1, 3))


def solution(mesh):
    return jax.shard_map(
        local,
        mesh=mesh,
        in_specs=(P(None, "gx", "gy", "gz"), P("gx", "gy", "gz")),
        out_specs=P(None, "gx", "gy", "gz"),
        check_vma=False,
    )
```

```python
import functools

import jax
import jax.numpy as jnp
import numpy as np
from jax import lax
from jax.experimental import pallas as pl
from jax.experimental.pallas import tpu as pltpu
from jax.sharding import PartitionSpec as P

MESH = pl.DeviceIdType.MESH
SECOND = (
    -5369.0 / 1800.0,
    12.0 / 7.0,
    -15.0 / 56.0,
    10.0 / 189.0,
    -1.0 / 112.0,
    2.0 / 1925.0,
    -1.0 / 16632.0,
)
FIRST = (6.0 / 7.0, -15.0 / 56.0, 5.0 / 63.0, -1.0 / 56.0, 3.0 / 385.0, -1.0 / 792.0)
G01, G02, G12 = 0.25, 0.15, 0.2
CENTER = 10.5
HALF_WIDTH = 9.5
SIGMA = -0.5 / HALF_WIDTH

XC = [SIGMA * c for c in SECOND]
XA = [SIGMA * 2.0 * G02 * a for a in FIRST]

F32 = jnp.float32
BF16 = jnp.bfloat16
STRIDE = 8
ROWS = 12 * STRIDE


def order_of_rows():
    rows = []
    for s in range(4):
        rows += [12 * s + r for r in range(8)]
    for s in range(4):
        rows += [12 * s + 8 + r for r in range(4)]
    return rows


def two_parts(m):
    hi = m.astype(np.float32).astype(jnp.bfloat16)
    lo = (m - hi.astype(np.float64)).astype(np.float32).astype(jnp.bfloat16)
    return hi, lo


def z_matrices():
    m = np.zeros((140, 256))
    for z in range(128):
        for k in range(1, 7):
            m[z + 6 + k, z] += FIRST[k - 1]
            m[z + 6 - k, z] -= FIRST[k - 1]
            m[z + 6 + k, 128 + z] += SIGMA * SECOND[k]
            m[z + 6 - k, 128 + z] += SIGMA * SECOND[k]
    inside = m[6:134]
    halo = np.zeros((128, 256))
    halo[122:128] = m[0:6]
    halo[0:6] = m[134:140]
    i1, i2 = two_parts(inside)
    h1, h2 = two_parts(halo)
    return np.stack([np.concatenate([i1, i1]), np.concatenate([i2, h1]), np.concatenate([h2, h1])])


def y_matrices():
    rows = order_of_rows()
    place = {y: r for r, y in enumerate(rows)}
    d1 = np.zeros((48, 48))
    d2 = np.zeros((48, 48))
    for y in range(48):
        for k in range(1, 7):
            d1[place[y], place[(y + k) % 48]] += FIRST[k - 1]
            d1[place[y], place[(y - k) % 48]] -= FIRST[k - 1]
            d2[place[y], place[(y + k) % 48]] += SECOND[k]
            d2[place[y], place[(y - k) % 48]] += SECOND[k]
    a1, a2 = two_parts(np.concatenate([(G01 / G02) * d1, SIGMA * d2]))
    b1, b2 = two_parts(SIGMA * 2.0 * G12 * d1)
    return np.concatenate([a1, a1, a2], axis=1), np.concatenate([b1, b1, b2], axis=1)


def split(value):
    hi = value.astype(BF16)
    lo = (value - hi.astype(F32)).astype(BF16)
    return hi, lo


def kernel(
    orb_hbm,
    pot_hbm,
    mz_hbm,
    my1_hbm,
    my2_hbm,
    out_hbm,
    orb,
    pot,
    mz,
    my1,
    my2,
    out,
    sm,
    sr,
    sz,
    spm,
    spr,
    v,
    rr,
    vp,
    vq,
    rp,
    zd,
    zs,
    zr,
    cs,
    cr,
    part,
    wf,
    v1,
    v2,
    h1,
    h2,
    tz,
    yf,
    ro,
    om,
    orr,
    load_s,
    tin_s,
    tin_r,
    zd_s,
    zd_r,
    zx_s,
    zx_r,
    xc_s,
    xc_r,
    to_s,
    to_r,
):
    gx = lax.axis_index("gx")
    gy = lax.axis_index("gy")
    gz = lax.axis_index("gz")
    half = gy // 2
    core = lax.rem(gy, 2)
    far = 1 - half
    near = [far * 2 + core, far * 2 + 1 - core, half * 2 + 1 - core]
    x_at = [{"gx": lax.rem(gx + 3, 4)}, {"gx": lax.rem(gx + 1, 4)}]
    z_to = [lax.rem(gz + 7, 8), lax.rem(gz + 1, 8)]
    z_at = [{"gz": z_to[0]}, {"gz": z_to[1]}]
    z_near = [gy] + near

    def copy(src, dst, send, recv, device):
        return pltpu.make_async_remote_copy(
            src_ref=src, dst_ref=dst, send_sem=send, recv_sem=recv, device_id=device, device_id_type=MESH
        )

    barrier = pltpu.get_barrier_semaphore()
    friends = x_at + [{"gy": n} for n in near]
    friends += [{"gy": n, "gz": z} for n in z_near for z in z_to]
    for device in friends:
        pl.semaphore_signal(barrier, inc=1, device_id=device, device_id_type=MESH)

    loads = [
        pltpu.make_async_copy(orb_hbm.at[:, 0], orb.at[0], load_s.at[0]),
        pltpu.make_async_copy(orb_hbm.at[:, 1], orb.at[1], load_s.at[1]),
        pltpu.make_async_copy(pot_hbm, pot, load_s.at[2]),
        pltpu.make_async_copy(mz_hbm, mz, load_s.at[3]),
        pltpu.make_async_copy(my1_hbm, my1, load_s.at[4]),
        pltpu.make_async_copy(my2_hbm, my2, load_s.at[5]),
    ]
    for one in loads:
        one.start()

    low_half = lax.broadcasted_iota(jnp.int32, (8, 128), 0) < 4
    lane8 = lax.broadcasted_iota(jnp.int32, (8, 128), 1)
    even_lane = lax.rem(lane8, 12) < 6
    lane = lax.broadcasted_iota(jnp.int32, (48, 128), 1)

    def turn(a):
        return pltpu.roll(a, 4, 0)

    def pair(a, b):
        return jnp.where(low_half, a, turn(b)), jnp.where(low_half, turn(a), b)

    def lanes(a, by):
        return a if by % 128 == 0 else pltpu.roll(a, by % 128, 1)

    orb_rows = orb.reshape(2304, 128)
    out_rows = out.reshape(2304, 128)
    started = []

    def start(c):
        c.start()
        started.append(c)

    def tin(c, rel):
        to = {"gy": near[rel]}
        return [
            copy(sm.at[c, near[rel]], v.at[c, 0, :, gy], tin_s.at[c, rel, 0], tin_r.at[c, rel, 0], to),
            copy(sr.at[c, near[rel]], rr.at[c, gy], tin_s.at[c, rel, 1], tin_r.at[c, rel, 1], to),
        ]

    def vin(rel):
        to = {"gy": near[rel]}
        return [
            copy(spm, vp.at[:, gy], tin_s.at[4, rel, 0], tin_r.at[4, rel, 0], to),
            copy(spr, rp.at[gy], tin_s.at[4, rel, 1], tin_r.at[4, rel, 1], to),
        ]

    def vpass():
        to = {"gy": near[2]}
        return [
            copy(vp.at[:, near[0]], vp.at[:, near[0]], tin_s.at[4, 1, 0], tin_r.at[4, 1, 0], to),
            copy(rp.at[near[0]], rp.at[near[0]], tin_s.at[4, 1, 1], tin_r.at[4, 1, 1], to),
        ]

    def zin(c, k, side):
        return copy(
            sz.at[c, z_near[k], side],
            zd.at[c, 1 - side, gy],
            zd_s.at[c, k, side],
            zd_r.at[c, k, side],
            {"gy": z_near[k], "gz": z_to[side]},
        )

    def prepare_potential():
        for x in range(12):
            spm[x] = pot[x, 0:8]
        for p in range(6):
            spr[p] = jnp.concatenate([pot[2 * p, 8:12], pot[2 * p + 1, 8:12]], axis=0)
        vp[:, gy] = spm[...]
        rp[gy] = spr[...]

    def prepare(c):
        def band(g, carry):
            b = 4 * (c % 2) + g
            main = [None] * 2
            rest = [None] * 4
            for x in range(12):
                val = orb_rows[pl.ds(1152 * (c // 2) + x * ROWS + b, 8, stride=STRIDE), :]
                sm[c, g, x] = val
                for side in range(2):
                    r = lanes(val, 6 * x + 6 * side)
                    main[side] = r if x == 0 else jnp.where(lane8 >= 6 * x, r, main[side])
            for p in range(6):
                lo = orb_rows[pl.ds(1152 * (c // 2) + 2 * p * ROWS + 8 * STRIDE + b, 4, stride=STRIDE), :]
                hi = orb_rows[pl.ds(1152 * (c // 2) + (2 * p + 1) * ROWS + 8 * STRIDE + b, 4, stride=STRIDE), :]
                val = jnp.concatenate([lo, hi], axis=0)
                sr[c, g, p] = val
                for side in range(2):
                    for odd in range(2):
                        r = lanes(val, 12 * p + 6 * odd + 6 * side)
                        at = 2 * side + odd
                        rest[at] = r if p == 0 else jnp.where(lane8 >= 12 * p + 6 * odd, r, rest[at])
            for side in range(2):
                sz[c, g, side, 0] = main[side]
                sz[c, g, side, 1] = jnp.where(low_half, rest[2 * side], rest[2 * side + 1])
            return carry

        lax.fori_loop(0, 4, band, 0)

    def send_in(c):
        for k in (1, 2, 0, 3):
            for side in range(2):
                start(zin(c, k, side))
        for rel in range(3):
            for one in tin(c, rel):
                start(one)
        v[c, 0, :, gy] = sm[c, gy]
        rr[c, gy] = sr[c, gy]

    def assemble(rest, dest):
        for p in range(6):
            for t in range(2):
                even, odd = pair(rest[2 * t, p], rest[2 * t + 1, p])
                dest(2 * p, 4 + t, even)
                dest(2 * p + 1, 4 + t, odd)

    def zx(c, side):
        return copy(zs.at[c, side], zr.at[c, 1 - side], zx_s.at[c, side], zx_r.at[c, side], z_at[side])

    def edges(c):
        low = None
        high = None
        for x in range(12):
            val = v[c, 1, x].reshape(48, 128)
            a = lanes(val, 6 * x)
            b = lanes(val, 6 * x + 6)
            low = a if x == 0 else jnp.where(lane >= 6 * x, a, low)
            high = b if x == 0 else jnp.where(lane >= 6 * x, b, high)
        zs[c, 0] = low.reshape(6, 8, 128)
        zs[c, 1] = high.reshape(6, 8, 128)
        for side in range(2):
            start(zx(c, side))

    def stage_a(c):
        for rel in range(3):
            for one in tin(c, rel):
                one.wait_recv()

        def dest(x, t, value):
            v[c, 0, x, t] = value

        assemble(rr.at[c], dest)

    def xc(c, step, side, piece):
        return copy(
            cs.at[c, step, side, piece],
            cr.at[c, step, side, piece],
            xc_s.at[c, step, side, piece],
            xc_r.at[c, step, side, piece],
            x_at[side],
        )

    def halo(c, step, side):
        if step == 1:
            zx(c, 1 - side).wait_recv()
            return zr[c, side].reshape(48, 128)
        for k in range(4):
            zin(c, k, 1 - side).wait_recv()
        tiles = [zd[c, side, s, 0] for s in range(4)]
        for t in range(2):
            a = zd[c, side, 2 * t, 1]
            b = zd[c, side, 2 * t + 1, 1]
            a = jnp.where(even_lane, a, turn(a))
            b = jnp.where(even_lane, turn(b), b)
            tiles.append(jnp.where(low_half, a, b))
        return jnp.concatenate(tiles, axis=0)

    def piece_tile(piece, i):
        block = far if piece == 0 else half
        return 2 * block + i if i < 2 else 4 + block

    def stage_b(c, step):
        for x in range(12):
            a, b = split(v[c, step, x].reshape(48, 128))
            v1[x] = a
            v2[x] = b
        below = halo(c, step, 0)
        above = halo(c, step, 1)
        for x in range(12):
            up = lanes(above, 128 - 6 * x)
            down = lanes(below, 122 - 6 * x)
            h = jnp.where(lane < 6, up, jnp.where(lane >= 122, down, 0.0))
            a, b = split(h)
            h1[x] = a
            h2[x] = b
        f1 = v1[...].reshape(576, 128)
        f2 = v2[...].reshape(576, 128)
        g1 = h1[...].reshape(576, 128)
        g2 = h2[...].reshape(576, 128)
        acc = jnp.dot(jnp.concatenate([f1, f2], axis=1), mz[0], preferred_element_type=F32)
        acc += jnp.dot(jnp.concatenate([f1, g1], axis=1), mz[1], preferred_element_type=F32)
        acc += jnp.dot(jnp.concatenate([g1, g2], axis=1), mz[2], preferred_element_type=F32)
        tz[...] = acc
        for xp in range(6):
            x0, x1 = 2 * xp, 2 * xp + 1
            a = jnp.concatenate([v1[x0], v1[x1]], axis=1)
            b = jnp.concatenate([v2[x0], v2[x1]], axis=1)
            q = jnp.dot(my1[...], jnp.concatenate([a, b, a], axis=0), preferred_element_type=F32)
            t = jnp.concatenate([tz[48 * x0 : 48 * x0 + 48, 0:128], tz[48 * x1 : 48 * x1 + 48, 0:128]], axis=1)
            s = jnp.concatenate([tz[48 * x0 : 48 * x0 + 48, 128:256], tz[48 * x1 : 48 * x1 + 48, 128:256]], axis=1)
            ta, tb = split(t)
            r = jnp.dot(my2[...], jnp.concatenate([ta, tb, ta], axis=0), preferred_element_type=F32)
            w = q[0:48] + t
            r = r + q[48:96] + s
            for i, x in enumerate((x0, x1)):
                wf[x] = w[:, 128 * i : 128 * i + 128].reshape(6, 8, 128)
                part[c, x] = r[:, 128 * i : 128 * i + 128].reshape(6, 8, 128)

        for piece in range(2):
            block = far if piece == 0 else half

            def tile(i, carry):
                t = (i // 2) * (4 + block) + (1 - i // 2) * (2 * block + i)
                acc = [None] * 24
                for j in range(12):
                    vj = v[c, step, j, t]
                    wj = wf[j, t]
                    for k in range(1, 7):
                        cv = XC[k] * vj
                        aw = XA[k - 1] * wj
                        lo, hi = j + 6 - k, j + 6 + k
                        acc[lo] = cv + aw if acc[lo] is None else acc[lo] + (cv + aw)
                        acc[hi] = cv - aw if acc[hi] is None else acc[hi] + (cv - aw)
                for j in range(6):
                    cs[c, step, 0, piece, j, i] = acc[j]
                    cs[c, step, 1, piece, j, i] = acc[18 + j]
                for j in range(12):
                    part[c, j, t] = part[c, j, t] + acc[6 + j]
                return carry

            lax.fori_loop(0, 3, tile, 0)
            for side in range(2):
                start(xc(c, step, side, piece))

    def to(c, rel):
        at = {"gy": near[rel]}
        return [
            copy(yf.at[c, :, near[rel]], om.at[c, gy], to_s.at[c, rel, 0], to_r.at[c, rel, 0], at),
            copy(ro.at[c, near[rel]], orr.at[c, gy], to_s.at[c, rel, 1], to_r.at[c, rel, 1], at),
        ]

    def stage_c(c, step):
        for piece in range(2):
            for side in range(2):
                xc(c, step, side, piece).wait_recv()
            for i in range(3):
                t = piece_tile(piece, i)
                got = jnp.concatenate([cr[c, step, 1, piece, :, i], cr[c, step, 0, piece, :, i]], axis=0)
                y = part[c, :, t] + got + vq[:, t] * v[c, step, :, t]
                if step == 0:
                    v[c, 1, :, t] = y
                else:
                    yf[c, :, t] = 2.0 * y - v[c, 0, :, t]
            if step == 0:
                continue
            block = far if piece == 0 else half
            for p in range(6):
                even, odd = pair(yf[c, 2 * p, 4 + block], yf[c, 2 * p + 1, 4 + block])
                ro[c, 2 * block, p] = even
                ro[c, 2 * block + 1, p] = odd
            for rel in (0, 1) if piece == 0 else (2,):
                for one in to(c, rel):
                    start(one)
        if step == 0:
            edges(c)
            return
        om[c, gy] = yf[c, :, gy]
        orr[c, gy] = ro[c, gy]

    def stage_d(c):
        for rel in (2, 0, 1):
            for one in to(c, rel):
                one.wait_recv()

        def band(g, carry):
            b = 4 * (c % 2) + g
            for x in range(12):
                out_rows[pl.ds(1152 * (c // 2) + x * ROWS + b, 8, stride=STRIDE), :] = om[c, g, x]
            for p in range(6):
                r = orr[c, g, p]
                out_rows[pl.ds(1152 * (c // 2) + 2 * p * ROWS + 8 * STRIDE + b, 4, stride=STRIDE), :] = r[0:4]
                out_rows[pl.ds(1152 * (c // 2) + (2 * p + 1) * ROWS + 8 * STRIDE + b, 4, stride=STRIDE), :] = r[4:8]
            return carry

        lax.fori_loop(0, 4, band, 0)

    def store(h):
        return pltpu.make_async_copy(out.at[h], out_hbm.at[:, h], load_s.at[6 + h])

    loads[0].wait()
    prepare(0)
    pl.semaphore_wait(barrier, len(friends))
    send_in(0)
    prepare(1)
    send_in(1)
    loads[2].wait()
    prepare_potential()
    for rel in (0, 2):
        for one in vin(rel):
            start(one)
    loads[1].wait()
    for c in (2, 3):
        prepare(c)
        send_in(c)
    for one in loads[3:]:
        one.wait()

    stage_a(0)
    stage_b(0, 0)
    stage_a(1)
    stage_b(1, 0)
    for one in vin(0):
        one.wait_recv()
    for one in vpass():
        start(one)
    for one in vin(2) + vpass():
        one.wait_recv()

    def scaled(a):
        return (a - CENTER) * (1.0 / HALF_WIDTH) + 3.0 * XC[0]

    def place(x, t, value):
        vq[x, t] = scaled(value)

    assemble(rp, place)
    for x in range(12):
        vq[x, 0:4] = scaled(vp[x])
    stage_c(0, 0)
    stage_a(2)
    stage_b(2, 0)
    stage_c(1, 0)
    stage_a(3)
    stage_b(3, 0)
    stage_b(0, 1)
    stage_c(2, 0)
    stage_b(1, 1)
    stage_c(3, 0)
    stage_b(2, 1)
    stage_c(0, 1)
    stage_b(3, 1)
    stage_c(1, 1)
    stage_c(2, 1)
    stage_d(0)
    stage_c(3, 1)
    stage_d(1)
    store(0).start()
    stage_d(2)
    stage_d(3)
    store(1).start()
    store(0).wait()
    store(1).wait()
    for one in started:
        one.wait_send()


def local(orbitals, potential):
    rows = jnp.transpose(orbitals, (1, 2, 0, 3)).reshape(144, 2, 8, 128)
    my1, my2 = y_matrices()
    anywhere = pl.BlockSpec(memory_space=pl.ANY)
    tile = (6, 8, 128)
    slab = (12, *tile)
    sem = pltpu.SemaphoreType.DMA

    def vmem(*shape, dtype=F32):
        return pltpu.VMEM(shape, dtype)

    out = pl.pallas_call(
        kernel,
        out_shape=jax.ShapeDtypeStruct((144, 2, 8, 128), F32),
        in_specs=[anywhere] * 5,
        out_specs=anywhere,
        scratch_shapes=[
            vmem(2, 144, 8, 128),
            vmem(12, 12, 128),
            vmem(3, 256, 256, dtype=BF16),
            vmem(96, 144, dtype=BF16),
            vmem(48, 144, dtype=BF16),
            vmem(2, 144, 8, 128),
            vmem(4, 4, 12, 8, 128),
            vmem(4, 4, *tile),
            vmem(4, 4, 2, 2, 8, 128),
            vmem(12, 8, 128),
            vmem(*tile),
            vmem(4, 2, *slab),
            vmem(4, 4, *tile),
            vmem(12, 4, 8, 128),
            vmem(*slab),
            vmem(4, *tile),
            vmem(4, 2, 4, 2, 8, 128),
            vmem(4, 2, *tile),
            vmem(4, 2, *tile),
            vmem(4, 2, 2, 2, 6, 3, 8, 128),
            vmem(4, 2, 2, 2, 6, 3, 8, 128),
            vmem(4, *slab),
            vmem(*slab),
            vmem(12, 48, 128, dtype=BF16),
            vmem(12, 48, 128, dtype=BF16),
            vmem(12, 48, 128, dtype=BF16),
            vmem(12, 48, 128, dtype=BF16),
            vmem(576, 256),
            vmem(4, *slab),
            vmem(4, 4, *tile),
            vmem(4, 4, 12, 8, 128),
            vmem(4, 4, *tile),
            sem((8,)),
            sem((5, 3, 2)),
            sem((5, 3, 2)),
            sem((4, 4, 2)),
            sem((4, 4, 2)),
            sem((4, 2)),
            sem((4, 2)),
            sem((4, 2, 2, 2)),
            sem((4, 2, 2, 2)),
            sem((4, 3, 2)),
            sem((4, 3, 2)),
        ],
        compiler_params=pltpu.CompilerParams(
            collective_id=0, has_side_effects=True, vmem_limit_bytes=60 * 1024 * 1024
        ),
    )(rows, potential, jnp.asarray(z_matrices()), jnp.asarray(my1), jnp.asarray(my2))
    return jnp.transpose(out.reshape(12, 12, 16, 128), (2, 0, 1, 3))


def solution(mesh):
    return jax.shard_map(
        local,
        mesh=mesh,
        in_specs=(P(None, "gx", "gy", "gz"), P("gx", "gy", "gz")),
        out_specs=P(None, "gx", "gy", "gz"),
        check_vma=False,
    )
```

```python
import functools

import jax
import jax.numpy as jnp
import numpy as np
from jax import lax
from jax.experimental import pallas as pl
from jax.experimental.pallas import tpu as pltpu
from jax.sharding import PartitionSpec as P

MESH = pl.DeviceIdType.MESH
SECOND = (
    -5369.0 / 1800.0,
    12.0 / 7.0,
    -15.0 / 56.0,
    10.0 / 189.0,
    -1.0 / 112.0,
    2.0 / 1925.0,
    -1.0 / 16632.0,
)
FIRST = (6.0 / 7.0, -15.0 / 56.0, 5.0 / 63.0, -1.0 / 56.0, 3.0 / 385.0, -1.0 / 792.0)
G01, G02, G12 = 0.25, 0.15, 0.2
CENTER = 10.5
HALF_WIDTH = 9.5
SIGMA = -0.5 / HALF_WIDTH

XC = [SIGMA * c for c in SECOND]
XA = [[SIGMA * 2.0 * g * a for a in FIRST] for g in (G02, G12)]

F32 = jnp.float32
BF16 = jnp.bfloat16


def order_of_rows():
    rows = []
    for s in range(4):
        rows += [12 * s + r for r in range(8)]
    for s in range(4):
        rows += [12 * s + 8 + r for r in range(4)]
    return rows


def two_parts(m):
    hi = m.astype(np.float32).astype(jnp.bfloat16)
    lo = (m - hi.astype(np.float64)).astype(np.float32).astype(jnp.bfloat16)
    return hi, lo


def z_matrices():
    m = np.zeros((140, 256))
    for z in range(128):
        for k in range(1, 7):
            m[z + 6 + k, z] += FIRST[k - 1]
            m[z + 6 - k, z] -= FIRST[k - 1]
            m[z + 6 + k, 128 + z] += SIGMA * SECOND[k]
            m[z + 6 - k, 128 + z] += SIGMA * SECOND[k]
    inside = m[6:134]
    halo = np.zeros((128, 256))
    halo[122:128] = m[0:6]
    halo[0:6] = m[134:140]
    i1, i2 = two_parts(inside)
    h1, h2 = two_parts(halo)
    return np.stack([np.concatenate([i1, i1]), np.concatenate([i2, h1]), np.concatenate([h2, h1])])


def y_matrices(g_here, g_other):
    rows = order_of_rows()
    place = {y: r for r, y in enumerate(rows)}
    d1 = np.zeros((48, 48))
    d2 = np.zeros((48, 48))
    for y in range(48):
        for k in range(1, 7):
            d1[place[y], place[(y + k) % 48]] += FIRST[k - 1]
            d1[place[y], place[(y - k) % 48]] -= FIRST[k - 1]
            d2[place[y], place[(y + k) % 48]] += SECOND[k]
            d2[place[y], place[(y - k) % 48]] += SECOND[k]
    a1, a2 = two_parts(np.concatenate([(G01 / g_here) * d1, SIGMA * d2]))
    b1, b2 = two_parts(SIGMA * 2.0 * g_other * d1)
    return np.concatenate([a1, a1, a2], axis=1), np.concatenate([b1, b1, b2], axis=1)


def split(value):
    hi = value.astype(BF16)
    lo = (value - hi.astype(F32)).astype(BF16)
    return hi, lo


def picked(c, g, i, rest):
    if c < 2:
        first, step = i * 96, 8
    else:
        first, step = 1152 + i * 8, 96
    first = first + 4 * (c % 2) + g
    return pl.ds(first + 8 * step, 4, stride=step) if rest else pl.ds(first, 8, stride=step)


def kernel(
    orb_hbm,
    pot_hbm,
    mz_hbm,
    my1_hbm,
    my2_hbm,
    om,
    orr,
    orb,
    pot,
    mz,
    my1,
    my2,
    sm,
    sr,
    sz,
    spm,
    spr,
    v,
    rr,
    vp,
    vq,
    rp,
    zd,
    zs,
    zr,
    cs,
    cr,
    part,
    wf,
    v1,
    v2,
    h1,
    h2,
    tz,
    yf,
    ro,
    load_s,
    sent,
    tin_r,
    vin_r,
    zd_r,
    zx_r,
    xc_r,
    to_r,
):
    gx = lax.axis_index("gx")
    gy = lax.axis_index("gy")
    gz = lax.axis_index("gz")
    axis = ("gy", "gx")
    pos = (gy, gx)
    half = [p // 2 for p in pos]
    core = [lax.rem(p, 2) for p in pos]
    far = [1 - h for h in half]
    near = [[f * 2 + k, f * 2 + 1 - k, h * 2 + 1 - k] for f, h, k in zip(far, half, core)]
    side_at = (
        ({"gx": lax.rem(gx + 3, 4)}, {"gx": lax.rem(gx + 1, 4)}),
        ({"gy": lax.rem(gy + 3, 4)}, {"gy": lax.rem(gy + 1, 4)}),
    )
    z_to = [lax.rem(gz + 7, 8), lax.rem(gz + 1, 8)]
    z_at = [{"gz": z_to[0]}, {"gz": z_to[1]}]
    z_near = [[pos[r]] + near[r] for r in range(2)]

    def copy(src, dst, send, recv, device):
        return pltpu.make_async_remote_copy(
            src_ref=src, dst_ref=dst, send_sem=send, recv_sem=recv, device_id=device, device_id_type=MESH
        )

    barrier = pltpu.get_barrier_semaphore()
    friends = [{axis[r]: n} for r in range(2) for n in near[r]]
    friends += z_at
    friends += [{axis[r]: n, "gz": z} for r in range(2) for n in near[r] for z in z_to]
    for device in friends:
        pl.semaphore_signal(barrier, inc=1, device_id=device, device_id_type=MESH)

    loads = [
        pltpu.make_async_copy(orb_hbm.at[:, 0], orb.at[0], load_s.at[0]),
        pltpu.make_async_copy(orb_hbm.at[:, 1], orb.at[1], load_s.at[1]),
        pltpu.make_async_copy(pot_hbm, pot, load_s.at[2]),
        pltpu.make_async_copy(mz_hbm, mz, load_s.at[3]),
        pltpu.make_async_copy(my1_hbm, my1, load_s.at[4]),
        pltpu.make_async_copy(my2_hbm, my2, load_s.at[5]),
    ]
    for one in loads:
        one.start()

    low_half = lax.broadcasted_iota(jnp.int32, (8, 128), 0) < 4
    lane8 = lax.broadcasted_iota(jnp.int32, (8, 128), 1)
    even_lane = lax.rem(lane8, 12) < 6
    lane = lax.broadcasted_iota(jnp.int32, (48, 128), 1)

    def turn(a):
        return pltpu.roll(a, 4, 0)

    def pair(a, b):
        return jnp.where(low_half, a, turn(b)), jnp.where(low_half, turn(a), b)

    def lanes(a, by):
        return a if by % 128 == 0 else pltpu.roll(a, by % 128, 1)

    orb_rows = orb.reshape(2304, 128)
    def start(c):
        c.start()

    def arrived(ref, sem):
        copy(ref, ref, sem, sem, {"gx": gx}).wait_recv()

    def tin(c, rel):
        r = c // 2
        peer = near[r][rel]
        to = {axis[r]: peer}
        return [
            copy(sm.at[c, peer], v.at[c, 0, :, pos[r]], sent.at[0], tin_r.at[c, 0], to),
            copy(sr.at[c, peer], rr.at[c, pos[r]], sent.at[1], tin_r.at[c, 1], to),
        ]

    def vin(r, rel):
        to = {axis[r]: near[r][rel]}
        return [
            copy(spm.at[r], vp.at[r, :, pos[r]], sent.at[2], vin_r.at[r, rel, 0], to),
            copy(spr.at[r], rp.at[r, pos[r]], sent.at[3], vin_r.at[r, rel, 1], to),
        ]

    def vpass(r):
        if r == 0:
            other, to = near[0][0], {"gy": near[0][2]}
            return [
                copy(vp.at[0, :, other], vp.at[0, :, other], sent.at[2], vin_r.at[0, 1, 0], to),
                copy(rp.at[0, other], rp.at[0, other], sent.at[3], vin_r.at[0, 1, 1], to),
            ]
        copies = []
        for k, (source, target) in enumerate(((1, 2), (2, 1))):
            other, to = near[1][source], {"gx": near[1][target]}
            lead, rest = vp.at[1, 6 * k : 6 * k + 6, other], rp.at[1, other, 3 * k : 3 * k + 3]
            copies.append(copy(lead, lead, sent.at[2], vin_r.at[1, 0, 0], to))
            copies.append(copy(rest, rest, sent.at[3], vin_r.at[1, 0, 1], to))
        return copies

    def zin(c, k, side):
        r = c // 2
        return copy(
            sz.at[c, z_near[r][k], side],
            zd.at[c, 1 - side, pos[r]],
            sent.at[4],
            zd_r.at[c],
            {axis[r]: z_near[r][k], "gz": z_to[side]},
        )

    def prepare_potential(r):
        def rows(i, start, count):
            if r == 0:
                return pot[i, start : start + count]
            return jnp.concatenate([pot[start + k, i : i + 1] for k in range(count)], axis=0)

        for i in range(12):
            spm[r, i] = rows(i, 0, 8)
        for p in range(6):
            spr[r, p] = jnp.concatenate([rows(2 * p, 8, 4), rows(2 * p + 1, 8, 4)], axis=0)
        vp[r, :, pos[r]] = spm[r]
        rp[r, pos[r]] = spr[r]

    def send_potential(r):
        for rel in (r, 2):
            for one in vin(r, rel):
                start(one)

    def pass_potential(r):
        for rel in (r, 2):
            for one in vin(r, rel):
                one.wait_recv()
        for one in vpass(r):
            start(one)

    def finish_potential(r):
        arrived(vp.at[r, :, 0], vin_r.at[r, 1 - r, 0])
        arrived(rp.at[r, 0], vin_r.at[r, 1 - r, 1])

        def scaled(a):
            return (a - CENTER) * (1.0 / HALF_WIDTH) + 3.0 * XC[0]

        def place(x, t, value):
            vq[r, x, t] = scaled(value)

        assemble(rp.at[r], place)
        for x in range(12):
            vq[r, x, 0:4] = scaled(vp[r, x])

    def prepare(c):
        def band(g, carry):
            main = [None] * 2
            rest = [None] * 4
            for x in range(12):
                val = orb_rows[picked(c, g, x, False), :]
                sm[c, g, x] = val
                for side in range(2):
                    r = lanes(val, 6 * x + 6 * side)
                    main[side] = r if x == 0 else jnp.where(lane8 >= 6 * x, r, main[side])
            for p in range(6):
                lo = orb_rows[picked(c, g, 2 * p, True), :]
                hi = orb_rows[picked(c, g, 2 * p + 1, True), :]
                val = jnp.concatenate([lo, hi], axis=0)
                sr[c, g, p] = val
                for side in range(2):
                    for odd in range(2):
                        r = lanes(val, 12 * p + 6 * odd + 6 * side)
                        at = 2 * side + odd
                        rest[at] = r if p == 0 else jnp.where(lane8 >= 12 * p + 6 * odd, r, rest[at])
            for side in range(2):
                sz[c, g, side, 0] = main[side]
                sz[c, g, side, 1] = jnp.where(low_half, rest[2 * side], rest[2 * side + 1])
            return carry

        lax.fori_loop(0, 4, band, 0)

    def send_in(c):
        for k in (1, 2, 0, 3):
            for side in range(2):
                start(zin(c, k, side))
        for rel in range(3):
            for one in tin(c, rel):
                start(one)
        me = pos[c // 2]
        v[c, 0, :, me] = sm[c, me]
        rr[c, me] = sr[c, me]

    def assemble(rest, dest):
        for p in range(6):
            for t in range(2):
                even, odd = pair(rest[2 * t, p], rest[2 * t + 1, p])
                dest(2 * p, 4 + t, even)
                dest(2 * p + 1, 4 + t, odd)

    def zx(c, side):
        return copy(zs.at[c, side], zr.at[c, 1 - side], sent.at[5], zx_r.at[c, side], z_at[side])

    def edges(c):
        low = None
        high = None
        for x in range(12):
            val = v[c, 1, x].reshape(48, 128)
            a = lanes(val, 6 * x)
            b = lanes(val, 6 * x + 6)
            low = a if x == 0 else jnp.where(lane >= 6 * x, a, low)
            high = b if x == 0 else jnp.where(lane >= 6 * x, b, high)
        zs[c, 0] = low.reshape(6, 8, 128)
        zs[c, 1] = high.reshape(6, 8, 128)
        for side in range(2):
            start(zx(c, side))

    def stage_a(c):
        arrived(v.at[c, 0, :, 0:3], tin_r.at[c, 0])
        arrived(rr.at[c, 0:3], tin_r.at[c, 1])

        def dest(x, t, value):
            v[c, 0, x, t] = value

        assemble(rr.at[c], dest)

    def xc(c, step, side, piece):
        return copy(
            cs.at[c, step, piece, side],
            cr.at[c, step, piece, side],
            sent.at[6],
            xc_r.at[c, step, piece],
            side_at[c // 2][side],
        )

    def halo(c, step, side):
        if step == 1:
            zx(c, 1 - side).wait_recv()
            return zr[c, side].reshape(48, 128)
        if side == 0:
            arrived(zd.at[c], zd_r.at[c])
        tiles = [zd[c, side, s, 0] for s in range(4)]
        for t in range(2):
            a = zd[c, side, 2 * t, 1]
            b = zd[c, side, 2 * t + 1, 1]
            a = jnp.where(even_lane, a, turn(a))
            b = jnp.where(even_lane, turn(b), b)
            tiles.append(jnp.where(low_half, a, b))
        return jnp.concatenate(tiles, axis=0)

    def block_of(c, piece):
        return far[c // 2] if piece == 0 else half[c // 2]

    def piece_tile(c, piece, i):
        block = block_of(c, piece)
        return 2 * block + i if i < 2 else 4 + block

    def stage_b(c, step, between=()):
        for x in range(12):
            a, b = split(v[c, step, x].reshape(48, 128))
            v1[x] = a
            v2[x] = b
        below = halo(c, step, 0)
        above = halo(c, step, 1)
        for x in range(12):
            up = lanes(above, 128 - 6 * x)
            down = lanes(below, 122 - 6 * x)
            h = jnp.where(lane < 6, up, jnp.where(lane >= 122, down, 0.0))
            a, b = split(h)
            h1[x] = a
            h2[x] = b
        for part_rows in range(2):
            xs = slice(6 * part_rows, 6 * part_rows + 6)
            f1 = v1[xs].reshape(288, 128)
            f2 = v2[xs].reshape(288, 128)
            g1 = h1[xs].reshape(288, 128)
            g2 = h2[xs].reshape(288, 128)
            acc = jnp.dot(jnp.concatenate([f1, f2], axis=1), mz[0], preferred_element_type=F32)
            acc += jnp.dot(jnp.concatenate([f1, g1], axis=1), mz[1], preferred_element_type=F32)
            acc += jnp.dot(jnp.concatenate([g1, g2], axis=1), mz[2], preferred_element_type=F32)
            tz[288 * part_rows : 288 * part_rows + 288] = acc
        for xp in range(6):
            x0, x1 = 2 * xp, 2 * xp + 1
            a = jnp.concatenate([v1[x0], v1[x1]], axis=1)
            b = jnp.concatenate([v2[x0], v2[x1]], axis=1)
            q = jnp.dot(my1[c // 2], jnp.concatenate([a, b, a], axis=0), preferred_element_type=F32)
            t = jnp.concatenate([tz[48 * x0 : 48 * x0 + 48, 0:128], tz[48 * x1 : 48 * x1 + 48, 0:128]], axis=1)
            s = jnp.concatenate([tz[48 * x0 : 48 * x0 + 48, 128:256], tz[48 * x1 : 48 * x1 + 48, 128:256]], axis=1)
            ta, tb = split(t)
            r = jnp.dot(my2[c // 2], jnp.concatenate([ta, tb, ta], axis=0), preferred_element_type=F32)
            w = q[0:48] + t
            r = r + q[48:96] + s
            for i, x in enumerate((x0, x1)):
                wf[x] = w[:, 128 * i : 128 * i + 128].reshape(6, 8, 128)
                part[c, x] = r[:, 128 * i : 128 * i + 128].reshape(6, 8, 128)

        for r in between:
            pass_potential(r)
        for piece in range(2):
            block = block_of(c, piece)

            def tile(i, carry):
                t = (i // 2) * (4 + block) + (1 - i // 2) * (2 * block + i)
                acc = [None] * 24
                for j in range(12):
                    vj = v[c, step, j, t]
                    wj = wf[j, t]
                    for k in range(1, 7):
                        cv = XC[k] * vj
                        aw = XA[c // 2][k - 1] * wj
                        lo, hi = j + 6 - k, j + 6 + k
                        acc[lo] = cv + aw if acc[lo] is None else acc[lo] + (cv + aw)
                        acc[hi] = cv - aw if acc[hi] is None else acc[hi] + (cv - aw)
                for j in range(6):
                    cs[c, step, piece, 0, j, i] = acc[j]
                    cs[c, step, piece, 1, j, i] = acc[18 + j]
                for j in range(12):
                    part[c, j, t] = part[c, j, t] + acc[6 + j]
                return carry

            lax.fori_loop(0, 3, tile, 0)
            for side in range(2):
                start(xc(c, step, side, piece))

    def to(c, rel):
        r = c // 2
        peer = near[r][rel]
        at = {axis[r]: peer}
        return [
            copy(yf.at[c, :, peer], om.at[c, pos[r]], sent.at[7], to_r.at[c, 0], at),
            copy(ro.at[c, peer], orr.at[c, pos[r]], sent.at[8], to_r.at[c, 1], at),
        ]

    def stage_c(c, step):
        for piece in range(2):
            arrived(cr.at[c, step, piece], xc_r.at[c, step, piece])
            for i in range(3):
                t = piece_tile(c, piece, i)
                got = jnp.concatenate([cr[c, step, piece, 1, :, i], cr[c, step, piece, 0, :, i]], axis=0)
                y = part[c, :, t] + got + vq[c // 2, :, t] * v[c, step, :, t]
                if step == 0:
                    v[c, 1, :, t] = y
                else:
                    yf[c, :, t] = 2.0 * y - v[c, 0, :, t]
            if step == 0:
                continue
            block = block_of(c, piece)
            for p in range(6):
                even, odd = pair(yf[c, 2 * p, 4 + block], yf[c, 2 * p + 1, 4 + block])
                ro[c, 2 * block, p] = even
                ro[c, 2 * block + 1, p] = odd
            for rel in (0, 1) if piece == 0 else (2,):
                for one in to(c, rel):
                    start(one)
        if step == 0:
            edges(c)
            return
        me = pos[c // 2]
        om[c, me] = yf[c, :, me]
        orr[c, me] = ro[c, me]

    def stage_d(c):
        arrived(om.at[c, 0:3], to_r.at[c, 0])
        arrived(orr.at[c, 0:3], to_r.at[c, 1])

    loads[0].wait()
    prepare(0)
    loads[1].wait()
    pl.semaphore_wait(barrier, len(friends))
    send_in(0)
    for c in (2, 1, 3):
        prepare(c)
        send_in(c)
    loads[2].wait()
    prepare_potential(0)
    send_potential(0)
    prepare_potential(1)
    send_potential(1)
    for one in loads[3:]:
        one.wait()

    stage_a(0)
    stage_b(0, 0)
    stage_a(2)
    stage_b(2, 0)
    stage_a(1)
    stage_b(1, 0, (0, 1))
    stage_a(3)
    stage_b(3, 0)
    finish_potential(0)
    stage_c(0, 0)
    finish_potential(1)
    stage_c(2, 0)
    stage_c(1, 0)
    stage_b(0, 1)
    stage_c(3, 0)
    stage_b(2, 1)
    stage_b(1, 1)
    stage_b(3, 1)
    stage_c(0, 1)
    stage_c(2, 1)
    stage_c(1, 1)
    stage_c(3, 1)
    for c in range(4):
        stage_d(c)
    done = [sm.at[:, 0:3], sr.at[:, 0:3], vp.at[:, :, 0:3], rp.at[:, 0:3], sz, zs, cs, yf.at[:, :, 0:3], ro.at[:, 0:3]]
    for i, ref in enumerate(done):
        copy(ref, ref, sent.at[i], sent.at[i], {"gx": gx}).wait_send()


def place_kernel(om, orr, out_hbm, out, store_s):
    out_rows = out.reshape(2304, 128)
    stores = [pltpu.make_async_copy(out.at[h], out_hbm.at[:, h], store_s.at[h]) for h in range(2)]
    for c in range(4):

        def band(g, carry):
            for x in range(12):
                out_rows[picked(c, g, x, False), :] = om[c, g, x]
            for p in range(6):
                r = orr[c, g, p]
                out_rows[picked(c, g, 2 * p, True), :] = r[0:4]
                out_rows[picked(c, g, 2 * p + 1, True), :] = r[4:8]
            return carry

        lax.fori_loop(0, 4, band, 0)
        if c % 2:
            stores[c // 2].start()
    for one in stores:
        one.wait()


def local(orbitals, potential):
    rows = jnp.transpose(orbitals, (1, 2, 0, 3)).reshape(144, 2, 8, 128)
    pairs = [y_matrices(G02, G12), y_matrices(G12, G02)]
    my1, my2 = (np.stack([p[i] for p in pairs]) for i in range(2))
    hbm = pl.BlockSpec(memory_space=pltpu.HBM)
    chip = pl.BlockSpec(memory_space=pltpu.VMEM)
    tile = (6, 8, 128)
    slab = (12, *tile)
    sem = pltpu.SemaphoreType.DMA

    def vmem(*shape, dtype=F32):
        return pltpu.VMEM(shape, dtype)

    inputs = [rows, potential, jnp.asarray(z_matrices()), jnp.asarray(my1), jnp.asarray(my2)]
    inputs = [pltpu.with_memory_space_constraint(a, pltpu.HBM) for a in inputs]
    main, rest = pl.pallas_call(
        kernel,
        out_shape=[jax.ShapeDtypeStruct((4, 4, 12, 8, 128), F32), jax.ShapeDtypeStruct((4, 4, *tile), F32)],
        in_specs=[hbm] * 5,
        out_specs=[chip] * 2,
        scratch_shapes=[
            vmem(2, 144, 8, 128),
            vmem(12, 12, 128),
            vmem(3, 256, 256, dtype=BF16),
            vmem(2, 96, 144, dtype=BF16),
            vmem(2, 48, 144, dtype=BF16),
            vmem(4, 4, 12, 8, 128),
            vmem(4, 4, *tile),
            vmem(4, 4, 2, 2, 8, 128),
            vmem(2, 12, 8, 128),
            vmem(2, *tile),
            vmem(4, 2, *slab),
            vmem(4, 4, *tile),
            vmem(2, 12, 4, 8, 128),
            vmem(2, *slab),
            vmem(2, 4, *tile),
            vmem(4, 2, 4, 2, 8, 128),
            vmem(4, 2, *tile),
            vmem(4, 2, *tile),
            vmem(4, 2, 2, 2, 6, 3, 8, 128),
            vmem(4, 2, 2, 2, 6, 3, 8, 128),
            vmem(4, *slab),
            vmem(*slab),
            vmem(12, 48, 128, dtype=BF16),
            vmem(12, 48, 128, dtype=BF16),
            vmem(12, 48, 128, dtype=BF16),
            vmem(12, 48, 128, dtype=BF16),
            vmem(576, 256),
            vmem(4, *slab),
            vmem(4, 4, *tile),
            sem((8,)),
            sem((9,)),
            sem((4, 2)),
            sem((2, 3, 2)),
            sem((4,)),
            sem((4, 2)),
            sem((4, 2, 2)),
            sem((4, 2)),
        ],
        compiler_params=pltpu.CompilerParams(
            collective_id=0, has_side_effects=True, vmem_limit_bytes=24 * 1024 * 1024
        ),
    )(*inputs)
    out = pl.pallas_call(
        place_kernel,
        out_shape=jax.ShapeDtypeStruct((144, 2, 8, 128), F32),
        in_specs=[chip] * 2,
        out_specs=hbm,
        scratch_shapes=[vmem(2, 144, 8, 128), sem((2,))],
        compiler_params=pltpu.CompilerParams(vmem_limit_bytes=8 * 1024 * 1024),
    )(main, rest)
    return jnp.transpose(out.reshape(12, 12, 16, 128), (2, 0, 1, 3))


def solution(mesh):
    return jax.shard_map(
        local,
        mesh=mesh,
        in_specs=(P(None, "gx", "gy", "gz"), P("gx", "gy", "gz")),
        out_specs=P(None, "gx", "gy", "gz"),
        check_vma=False,
    )
```

```python
import functools

import jax
import jax.numpy as jnp
import numpy as np
from jax import lax
from jax.experimental import pallas as pl
from jax.experimental.pallas import tpu as pltpu
from jax.sharding import PartitionSpec as P

MESH = pl.DeviceIdType.MESH
SECOND = (
    -5369.0 / 1800.0,
    12.0 / 7.0,
    -15.0 / 56.0,
    10.0 / 189.0,
    -1.0 / 112.0,
    2.0 / 1925.0,
    -1.0 / 16632.0,
)
FIRST = (6.0 / 7.0, -15.0 / 56.0, 5.0 / 63.0, -1.0 / 56.0, 3.0 / 385.0, -1.0 / 792.0)
G01, G02, G12 = 0.25, 0.15, 0.2
CENTER = 10.5
HALF_WIDTH = 9.5
SIGMA = -0.5 / HALF_WIDTH

XC = [SIGMA * c for c in SECOND]
XA = [[SIGMA * 2.0 * g * a for a in FIRST] for g in (G02, G12)]

F32 = jnp.float32
BF16 = jnp.bfloat16


def order_of_rows():
    rows = []
    for s in range(4):
        rows += [12 * s + r for r in range(8)]
    for s in range(4):
        rows += [12 * s + 8 + r for r in range(4)]
    return rows


def two_parts(m):
    hi = m.astype(np.float32).astype(jnp.bfloat16)
    lo = (m - hi.astype(np.float64)).astype(np.float32).astype(jnp.bfloat16)
    return hi, lo


def z_matrices():
    m = np.zeros((140, 256))
    for z in range(128):
        for k in range(1, 7):
            m[z + 6 + k, z] += FIRST[k - 1]
            m[z + 6 - k, z] -= FIRST[k - 1]
            m[z + 6 + k, 128 + z] += SIGMA * SECOND[k]
            m[z + 6 - k, 128 + z] += SIGMA * SECOND[k]
    inside = m[6:134]
    halo = np.zeros((128, 256))
    halo[122:128] = m[0:6]
    halo[0:6] = m[134:140]
    i1, i2 = two_parts(inside)
    h1, h2 = two_parts(halo)
    return np.stack([np.concatenate([i1, i1]), np.concatenate([i2, h1]), np.concatenate([h2, h1])])


def y_matrices(g_here, g_other):
    rows = order_of_rows()
    place = {y: r for r, y in enumerate(rows)}
    d1 = np.zeros((48, 48))
    d2 = np.zeros((48, 48))
    for y in range(48):
        for k in range(1, 7):
            d1[place[y], place[(y + k) % 48]] += FIRST[k - 1]
            d1[place[y], place[(y - k) % 48]] -= FIRST[k - 1]
            d2[place[y], place[(y + k) % 48]] += SECOND[k]
            d2[place[y], place[(y - k) % 48]] += SECOND[k]
    a1, a2 = two_parts(np.concatenate([(G01 / g_here) * d1, SIGMA * d2]))
    b1, b2 = two_parts(SIGMA * 2.0 * g_other * d1)
    return np.concatenate([a1, a1, a2], axis=1), np.concatenate([b1, b1, b2], axis=1)


def split(value):
    hi = value.astype(BF16)
    lo = (value - hi.astype(F32)).astype(BF16)
    return hi, lo


def picked(c, g, i, rest):
    if c < 2:
        first, step = i * 96, 8
    else:
        first, step = 1152 + i * 8, 96
    first = first + 4 * (c % 2) + g
    return pl.ds(first + 8 * step, 4, stride=step) if rest else pl.ds(first, 8, stride=step)


def kernel(
    orb_hbm,
    pot_hbm,
    mz_hbm,
    my1_hbm,
    my2_hbm,
    out,
    orb,
    pot,
    mz,
    my1,
    my2,
    sm,
    sr,
    sz,
    spm,
    spr,
    v,
    rr,
    vp,
    vq,
    rp,
    zd,
    zs,
    zr,
    cs,
    cr,
    part,
    wf,
    v1,
    v2,
    h1,
    h2,
    tz,
    yf,
    ro,
    om,
    orr,
    load_s,
    sent,
    tin_r,
    vin_r,
    zd_r,
    zx_r,
    xc_r,
    to_r,
):
    gx = lax.axis_index("gx")
    gy = lax.axis_index("gy")
    gz = lax.axis_index("gz")
    axis = ("gy", "gx")
    pos = (gy, gx)
    half = [p // 2 for p in pos]
    core = [lax.rem(p, 2) for p in pos]
    far = [1 - h for h in half]
    near = [[f * 2 + k, f * 2 + 1 - k, h * 2 + 1 - k] for f, h, k in zip(far, half, core)]
    side_at = (
        ({"gx": lax.rem(gx + 3, 4)}, {"gx": lax.rem(gx + 1, 4)}),
        ({"gy": lax.rem(gy + 3, 4)}, {"gy": lax.rem(gy + 1, 4)}),
    )
    z_to = [lax.rem(gz + 7, 8), lax.rem(gz + 1, 8)]
    z_at = [{"gz": z_to[0]}, {"gz": z_to[1]}]
    z_near = [[pos[r]] + near[r] for r in range(2)]

    def copy(src, dst, send, recv, device):
        return pltpu.make_async_remote_copy(
            src_ref=src, dst_ref=dst, send_sem=send, recv_sem=recv, device_id=device, device_id_type=MESH
        )

    barrier = pltpu.get_barrier_semaphore()
    friends = [{axis[r]: n} for r in range(2) for n in near[r]]
    friends += z_at
    friends += [{axis[r]: n, "gz": z} for r in range(2) for n in near[r] for z in z_to]
    for device in friends:
        pl.semaphore_signal(barrier, inc=1, device_id=device, device_id_type=MESH)

    loads = [
        pltpu.make_async_copy(orb_hbm.at[:, 0], orb.at[0], load_s.at[0]),
        pltpu.make_async_copy(orb_hbm.at[:, 1], orb.at[1], load_s.at[1]),
        pltpu.make_async_copy(pot_hbm, pot, load_s.at[2]),
        pltpu.make_async_copy(mz_hbm, mz, load_s.at[3]),
        pltpu.make_async_copy(my1_hbm, my1, load_s.at[4]),
        pltpu.make_async_copy(my2_hbm, my2, load_s.at[5]),
    ]
    for one in loads:
        one.start()

    low_half = lax.broadcasted_iota(jnp.int32, (8, 128), 0) < 4
    lane8 = lax.broadcasted_iota(jnp.int32, (8, 128), 1)
    lane = lax.broadcasted_iota(jnp.int32, (48, 128), 1)

    def turn(a):
        return pltpu.roll(a, 4, 0)

    def pair(a, b):
        return jnp.where(low_half, a, turn(b)), jnp.where(low_half, turn(a), b)

    def lanes(a, by):
        return a if by % 128 == 0 else pltpu.roll(a, by % 128, 1)

    orb_rows = orb.reshape(2304, 128)
    out_rows = out.reshape(2304, 128)
    def start(c):
        c.start()

    def arrived(ref, sem):
        copy(ref, ref, sem, sem, {"gx": gx}).wait_recv()

    def tin(c, rel):
        r = c // 2
        peer = near[r][rel]
        to = {axis[r]: peer}
        return [
            copy(sm.at[c, peer], v.at[c, 0, :, pos[r]], sent.at[0], tin_r.at[c, 0], to),
            copy(sr.at[c, peer], rr.at[c, pos[r]], sent.at[1], tin_r.at[c, 1], to),
        ]

    def vin(r, rel):
        to = {axis[r]: near[r][rel]}
        return [
            copy(spm.at[r], vp.at[r, :, pos[r]], sent.at[2], vin_r.at[r, rel, 0], to),
            copy(spr.at[r], rp.at[r, pos[r]], sent.at[3], vin_r.at[r, rel, 1], to),
        ]

    def vpass():
        other, to = near[0][0], {"gy": near[0][2]}
        return [
            copy(vp.at[0, :, other], vp.at[0, :, other], sent.at[2], vin_r.at[0, 1, 0], to),
            copy(rp.at[0, other], rp.at[0, other], sent.at[3], vin_r.at[0, 1, 1], to),
        ]

    def zin(c, k, side):
        r = c // 2
        return copy(
            sz.at[c, z_near[r][k], side],
            zd.at[c, 1 - side, pos[r]],
            sent.at[4],
            zd_r.at[c],
            {axis[r]: z_near[r][k], "gz": z_to[side]},
        )

    def prepare_potential(r):
        def rows(i, start, count):
            if r == 0:
                return pot[i, start : start + count]
            return jnp.concatenate([pot[start + k, i : i + 1] for k in range(count)], axis=0)

        for i in range(12):
            spm[r, i] = rows(i, 0, 8)
        for p in range(6):
            spr[r, p] = jnp.concatenate([rows(2 * p, 8, 4), rows(2 * p + 1, 8, 4)], axis=0)
        vp[r, :, pos[r]] = spm[r]
        rp[r, pos[r]] = spr[r]

    def send_potential(r):
        for rel in ((0, 2), (1, 2, 0))[r]:
            for one in vin(r, rel):
                start(one)

    def pass_potential():
        for rel in (0, 2):
            for one in vin(0, rel):
                one.wait_recv()
        for one in vpass():
            start(one)

    def finish_potential(r):
        for one in vpass() if r == 0 else vin(1, 0) + vin(1, 1) + vin(1, 2):
            one.wait_recv()

        def scaled(a):
            return (a - CENTER) * (1.0 / HALF_WIDTH) + 3.0 * XC[0]

        def place(x, t, value):
            vq[r, x, t] = scaled(value)

        assemble(rp.at[r], place)
        for x in range(12):
            vq[r, x, 0:4] = scaled(vp[r, x])

    def prepare(c):
        def band(g, carry):
            edge = [None] * 2
            for x in range(12):
                val = orb_rows[picked(c, g, x, False), :]
                sm[c, g, x] = val
                for side in range(2):
                    r = lanes(val, 6 * x + 6 * side)
                    edge[side] = r if x == 0 else jnp.where(lane8 >= 6 * x, r, edge[side])
            for p in range(6):
                lo = orb_rows[picked(c, g, 2 * p, True), :]
                hi = orb_rows[picked(c, g, 2 * p + 1, True), :]
                val = jnp.concatenate([lo, hi], axis=0)
                sr[c, g, p] = val
                for side in range(2):
                    r = lanes(val, 72 + 6 * p + 6 * side)
                    edge[side] = jnp.where(lane8 >= 72 + 6 * p, r, edge[side])
            for side in range(2):
                sz[c, g, side] = edge[side]
            return carry

        lax.fori_loop(0, 4, band, 0)

    def send_in(c):
        for k in (1, 2, 0, 3):
            for side in range(2):
                start(zin(c, k, side))
        for rel in range(3):
            for one in tin(c, rel):
                start(one)
        me = pos[c // 2]
        v[c, 0, :, me] = sm[c, me]
        rr[c, me] = sr[c, me]

    def assemble(rest, dest):
        for p in range(6):
            for t in range(2):
                even, odd = pair(rest[2 * t, p], rest[2 * t + 1, p])
                dest(2 * p, 4 + t, even)
                dest(2 * p + 1, 4 + t, odd)

    def zx(c, side):
        return copy(zs.at[c, side], zr.at[c, 1 - side], sent.at[5], zx_r.at[c, side], z_at[side])

    def edges(c):
        low = None
        high = None
        for x in range(12):
            val = v[c, 1, x].reshape(48, 128)
            a = lanes(val, 6 * x)
            b = lanes(val, 6 * x + 6)
            low = a if x == 0 else jnp.where(lane >= 6 * x, a, low)
            high = b if x == 0 else jnp.where(lane >= 6 * x, b, high)
        zs[c, 0] = low.reshape(6, 8, 128)
        zs[c, 1] = high.reshape(6, 8, 128)
        for side in range(2):
            start(zx(c, side))

    def stage_a(c):
        arrived(v.at[c, 0, :, 0:3], tin_r.at[c, 0])
        arrived(rr.at[c, 0:3], tin_r.at[c, 1])

        def dest(x, t, value):
            v[c, 0, x, t] = value

        assemble(rr.at[c], dest)

    def xc(c, step, side, piece):
        return copy(
            cs.at[c, step, piece, side],
            cr.at[c, step, piece, side],
            sent.at[6],
            xc_r.at[c, step, piece],
            side_at[c // 2][side],
        )

    def halo(c, step):
        if step == 1:
            for side in range(2):
                zx(c, side).wait_recv()
            far_side = [zr[c, side].reshape(48, 128) for side in range(2)]
            return lambda side, x, by: lanes(far_side[side], by - 6 * x)
        arrived(zd.at[c], zd_r.at[c])
        main = []
        rest = []
        for side in range(2):
            tiles = [zd[c, side, s] for s in range(4)]
            main.append(jnp.concatenate(tiles, axis=0))
            both = [pair(tiles[2 * t], tiles[2 * t + 1]) for t in range(2)]
            rest.append([jnp.concatenate([both[0][k], both[1][k]], axis=0) for k in range(2)])

        def edge(side, x, by):
            a = lanes(main[side], by - 6 * x)
            b = lanes(rest[side][x % 2], by - 72 - 6 * (x // 2))
            return jnp.concatenate([a, b], axis=0)

        return edge

    def block_of(c, piece):
        return far[c // 2] if piece == 0 else half[c // 2]

    def piece_tile(c, piece, i):
        block = block_of(c, piece)
        return 2 * block + i if i < 2 else 4 + block

    def stage_b(c, step):
        for x in range(12):
            a, b = split(v[c, step, x].reshape(48, 128))
            v1[x] = a
            v2[x] = b
        edge = halo(c, step)
        for x in range(12):
            up = edge(1, x, 128)
            down = edge(0, x, 122)
            h = jnp.where(lane < 6, up, jnp.where(lane >= 122, down, 0.0))
            a, b = split(h)
            h1[x] = a
            h2[x] = b
        for part_rows in range(2):
            xs = slice(6 * part_rows, 6 * part_rows + 6)
            f1 = v1[xs].reshape(288, 128)
            f2 = v2[xs].reshape(288, 128)
            g1 = h1[xs].reshape(288, 128)
            g2 = h2[xs].reshape(288, 128)
            acc = jnp.dot(jnp.concatenate([f1, f2], axis=1), mz[0], preferred_element_type=F32)
            acc += jnp.dot(jnp.concatenate([f1, g1], axis=1), mz[1], preferred_element_type=F32)
            acc += jnp.dot(jnp.concatenate([g1, g2], axis=1), mz[2], preferred_element_type=F32)
            tz[288 * part_rows : 288 * part_rows + 288] = acc
        for xp in range(6):
            x0, x1 = 2 * xp, 2 * xp + 1
            a = jnp.concatenate([v1[x0], v1[x1]], axis=1)
            b = jnp.concatenate([v2[x0], v2[x1]], axis=1)
            q = jnp.dot(my1[c // 2], jnp.concatenate([a, b, a], axis=0), preferred_element_type=F32)
            t = jnp.concatenate([tz[48 * x0 : 48 * x0 + 48, 0:128], tz[48 * x1 : 48 * x1 + 48, 0:128]], axis=1)
            s = jnp.concatenate([tz[48 * x0 : 48 * x0 + 48, 128:256], tz[48 * x1 : 48 * x1 + 48, 128:256]], axis=1)
            ta, tb = split(t)
            r = jnp.dot(my2[c // 2], jnp.concatenate([ta, tb, ta], axis=0), preferred_element_type=F32)
            w = q[0:48] + t
            r = r + q[48:96] + s
            for i, x in enumerate((x0, x1)):
                wf[x] = w[:, 128 * i : 128 * i + 128].reshape(6, 8, 128)
                part[c, x] = r[:, 128 * i : 128 * i + 128].reshape(6, 8, 128)

        for piece in range(2):
            block = block_of(c, piece)

            def tile(i, carry):
                t = (i // 2) * (4 + block) + (1 - i // 2) * (2 * block + i)
                acc = [None] * 24
                for j in range(12):
                    vj = v[c, step, j, t]
                    wj = wf[j, t]
                    for k in range(1, 7):
                        cv = XC[k] * vj
                        aw = XA[c // 2][k - 1] * wj
                        lo, hi = j + 6 - k, j + 6 + k
                        acc[lo] = cv + aw if acc[lo] is None else acc[lo] + (cv + aw)
                        acc[hi] = cv - aw if acc[hi] is None else acc[hi] + (cv - aw)
                for j in range(6):
                    cs[c, step, piece, 0, j, i] = acc[j]
                    cs[c, step, piece, 1, j, i] = acc[18 + j]
                for j in range(12):
                    part[c, j, t] = part[c, j, t] + acc[6 + j]
                return carry

            lax.fori_loop(0, 3, tile, 0, unroll=True)
            for side in range(2):
                start(xc(c, step, side, piece))

    def to(c, rel):
        r = c // 2
        peer = near[r][rel]
        at = {axis[r]: peer}
        return [
            copy(yf.at[c, :, peer], om.at[c, pos[r]], sent.at[7], to_r.at[c, 0], at),
            copy(ro.at[c, peer], orr.at[c, pos[r]], sent.at[8], to_r.at[c, 1], at),
        ]

    def stage_c(c, step):
        for piece in range(2):
            arrived(cr.at[c, step, piece], xc_r.at[c, step, piece])
            for i in range(3):
                t = piece_tile(c, piece, i)
                got = jnp.concatenate([cr[c, step, piece, 1, :, i], cr[c, step, piece, 0, :, i]], axis=0)
                y = part[c, :, t] + got + vq[c // 2, :, t] * v[c, step, :, t]
                if step == 0:
                    v[c, 1, :, t] = y
                else:
                    yf[c, :, t] = 2.0 * y - v[c, 0, :, t]
            if step == 0:
                continue
            block = block_of(c, piece)
            for p in range(6):
                even, odd = pair(yf[c, 2 * p, 4 + block], yf[c, 2 * p + 1, 4 + block])
                ro[c, 2 * block, p] = even
                ro[c, 2 * block + 1, p] = odd
            for rel in (0, 1) if piece == 0 else (2,):
                for one in to(c, rel):
                    start(one)
        if step == 0:
            edges(c)
            return
        me = pos[c // 2]
        om[c, me] = yf[c, :, me]
        orr[c, me] = ro[c, me]

    def stage_d(c):
        arrived(om.at[c, 0:3], to_r.at[c, 0])
        arrived(orr.at[c, 0:3], to_r.at[c, 1])

        def band(g, carry):
            for x in range(12):
                out_rows[picked(c, g, x, False), :] = om[c, g, x]
            for p in range(6):
                r = orr[c, g, p]
                out_rows[picked(c, g, 2 * p, True), :] = r[0:4]
                out_rows[picked(c, g, 2 * p + 1, True), :] = r[4:8]
            return carry

        lax.fori_loop(0, 4, band, 0)

    loads[0].wait()
    prepare(0)
    loads[1].wait()
    pl.semaphore_wait(barrier, len(friends))
    send_in(0)
    for c in (2, 1, 3):
        prepare(c)
        send_in(c)
    loads[2].wait()
    prepare_potential(0)
    send_potential(0)
    prepare_potential(1)
    for one in loads[3:]:
        one.wait()

    send_potential(1)
    stage_a(0)
    stage_b(0, 0)
    stage_a(2)
    stage_b(2, 0)
    stage_a(1)
    stage_b(1, 0)
    pass_potential()
    stage_a(3)
    stage_b(3, 0)
    finish_potential(0)
    finish_potential(1)
    stage_c(2, 0)
    stage_c(0, 0)
    stage_c(3, 0)
    stage_b(2, 1)
    stage_c(1, 0)
    stage_b(0, 1)
    stage_b(3, 1)
    stage_b(1, 1)
    stage_c(2, 1)
    stage_c(0, 1)
    stage_c(3, 1)
    stage_c(1, 1)
    for c in (2, 0, 3, 1):
        stage_d(c)
    done = [sm.at[:, 0:3], sr.at[:, 0:3], vp.at[:, :, 0:3], rp.at[:, 0:3], sz, zs, cs, yf.at[:, :, 0:3], ro.at[:, 0:3]]
    for i, ref in enumerate(done):
        copy(ref, ref, sent.at[i], sent.at[i], {"gx": gx}).wait_send()


def place_kernel(out, out_hbm, store_s):
    stores = [
        pltpu.make_async_copy(out.at[h, 36 * k : 36 * k + 36], out_hbm.at[36 * k : 36 * k + 36, h], store_s.at[h, k])
        for h in range(2)
        for k in range(4)
    ]
    for one in stores:
        one.start()
    for one in stores:
        one.wait()


def local(orbitals, potential):
    rows = jnp.transpose(orbitals, (1, 2, 0, 3)).reshape(144, 2, 8, 128)
    pairs = [y_matrices(G02, G12), y_matrices(G12, G02)]
    my1, my2 = (np.stack([p[i] for p in pairs]) for i in range(2))
    hbm = pl.BlockSpec(memory_space=pltpu.HBM)
    chip = pl.BlockSpec(memory_space=pltpu.VMEM)
    tile = (6, 8, 128)
    slab = (12, *tile)
    sem = pltpu.SemaphoreType.DMA

    def vmem(*shape, dtype=F32):
        return pltpu.VMEM(shape, dtype)

    inputs = [rows, potential, jnp.asarray(z_matrices()), jnp.asarray(my1), jnp.asarray(my2)]
    inputs = [pltpu.with_memory_space_constraint(a, pltpu.HBM) for a in inputs]
    placed = pl.pallas_call(
        kernel,
        out_shape=jax.ShapeDtypeStruct((2, 144, 8, 128), F32),
        in_specs=[hbm] * 5,
        out_specs=chip,
        scratch_shapes=[
            vmem(2, 144, 8, 128),
            vmem(12, 12, 128),
            vmem(3, 256, 256, dtype=BF16),
            vmem(2, 96, 144, dtype=BF16),
            vmem(2, 48, 144, dtype=BF16),
            vmem(4, 4, 12, 8, 128),
            vmem(4, 4, *tile),
            vmem(4, 4, 2, 8, 128),
            vmem(2, 12, 8, 128),
            vmem(2, *tile),
            vmem(4, 2, *slab),
            vmem(4, 4, *tile),
            vmem(2, 12, 4, 8, 128),
            vmem(2, *slab),
            vmem(2, 4, *tile),
            vmem(4, 2, 4, 8, 128),
            vmem(4, 2, *tile),
            vmem(4, 2, *tile),
            vmem(4, 2, 2, 2, 6, 3, 8, 128),
            vmem(4, 2, 2, 2, 6, 3, 8, 128),
            vmem(4, *slab),
            vmem(*slab),
            vmem(12, 48, 128, dtype=BF16),
            vmem(12, 48, 128, dtype=BF16),
            vmem(12, 48, 128, dtype=BF16),
            vmem(12, 48, 128, dtype=BF16),
            vmem(576, 256),
            vmem(4, *slab),
            vmem(4, 4, *tile),
            vmem(4, 4, 12, 8, 128),
            vmem(4, 4, *tile),
            sem((8,)),
            sem((9,)),
            sem((4, 2)),
            sem((2, 3, 2)),
            sem((4,)),
            sem((4, 2)),
            sem((4, 2, 2)),
            sem((4, 2)),
        ],
        compiler_params=pltpu.CompilerParams(
            collective_id=0, has_side_effects=True, vmem_limit_bytes=24 * 1024 * 1024
        ),
    )(*inputs)
    out = pl.pallas_call(
        place_kernel,
        out_shape=jax.ShapeDtypeStruct((144, 2, 8, 128), F32),
        in_specs=[chip],
        out_specs=hbm,
        scratch_shapes=[sem((2, 4))],
        compiler_params=pltpu.CompilerParams(vmem_limit_bytes=8 * 1024 * 1024),
    )(placed)
    return jnp.transpose(out.reshape(12, 12, 16, 128), (2, 0, 1, 3))


def solution(mesh):
    return jax.shard_map(
        local,
        mesh=mesh,
        in_specs=(P(None, "gx", "gy", "gz"), P("gx", "gy", "gz")),
        out_specs=P(None, "gx", "gy", "gz"),
        check_vma=False,
    )
```

```python
import functools

import jax
import jax.numpy as jnp
import numpy as np
from jax import lax
from jax.experimental import pallas as pl
from jax.experimental.pallas import tpu as pltpu
from jax.sharding import PartitionSpec as P

MESH = pl.DeviceIdType.MESH
SECOND = (
    -5369.0 / 1800.0,
    12.0 / 7.0,
    -15.0 / 56.0,
    10.0 / 189.0,
    -1.0 / 112.0,
    2.0 / 1925.0,
    -1.0 / 16632.0,
)
FIRST = (6.0 / 7.0, -15.0 / 56.0, 5.0 / 63.0, -1.0 / 56.0, 3.0 / 385.0, -1.0 / 792.0)
G01, G02, G12 = 0.25, 0.15, 0.2
CENTER = 10.5
HALF_WIDTH = 9.5
SIGMA = -0.5 / HALF_WIDTH

XC = [SIGMA * c for c in SECOND]
XA = [[SIGMA * 2.0 * g * a for a in FIRST] for g in (G02, G12)]

F32 = jnp.float32
BF16 = jnp.bfloat16


def order_of_rows():
    rows = []
    for s in range(4):
        rows += [12 * s + r for r in range(8)]
    for s in range(4):
        rows += [12 * s + 8 + r for r in range(4)]
    return rows


def two_parts(m):
    hi = m.astype(np.float32).astype(jnp.bfloat16)
    lo = (m - hi.astype(np.float64)).astype(np.float32).astype(jnp.bfloat16)
    return hi, lo


def z_matrices():
    m = np.zeros((140, 256))
    for z in range(128):
        for k in range(1, 7):
            m[z + 6 + k, z] += FIRST[k - 1]
            m[z + 6 - k, z] -= FIRST[k - 1]
            m[z + 6 + k, 128 + z] += SIGMA * SECOND[k]
            m[z + 6 - k, 128 + z] += SIGMA * SECOND[k]
    inside = m[6:134]
    halo = np.zeros((128, 256))
    halo[122:128] = m[0:6]
    halo[0:6] = m[134:140]
    i1, i2 = two_parts(inside)
    h1, h2 = two_parts(halo)
    return np.stack([np.concatenate([i1, i1]), np.concatenate([i2, h1]), np.concatenate([h2, h1])])


def y_matrices(g_here, g_other):
    rows = order_of_rows()
    place = {y: r for r, y in enumerate(rows)}
    d1 = np.zeros((48, 48))
    d2 = np.zeros((48, 48))
    for y in range(48):
        for k in range(1, 7):
            d1[place[y], place[(y + k) % 48]] += FIRST[k - 1]
            d1[place[y], place[(y - k) % 48]] -= FIRST[k - 1]
            d2[place[y], place[(y + k) % 48]] += SECOND[k]
            d2[place[y], place[(y - k) % 48]] += SECOND[k]
    a1, a2 = two_parts(np.concatenate([(G01 / g_here) * d1, SIGMA * d2]))
    b1, b2 = two_parts(SIGMA * 2.0 * g_other * d1)
    return np.concatenate([a1, a1, a2], axis=1), np.concatenate([b1, b1, b2], axis=1)


def split(value):
    hi = value.astype(BF16)
    lo = (value - hi.astype(F32)).astype(BF16)
    return hi, lo


def picked(c, g, i, rest):
    if c < 2:
        first, step = i * 96, 8
    else:
        first, step = 1152 + i * 8, 96
    first = first + 4 * (c % 2) + g
    return pl.ds(first + 8 * step, 4, stride=step) if rest else pl.ds(first, 8, stride=step)


def kernel(
    orb_hbm,
    pot_hbm,
    mz_hbm,
    my1_hbm,
    my2_hbm,
    out,
    orb,
    pot,
    mz,
    my1,
    my2,
    sm,
    sr,
    sz,
    spm,
    spr,
    v,
    rr,
    vp,
    vq,
    rp,
    zd,
    zs,
    zr,
    cs,
    cr,
    part,
    wf,
    v1,
    v2,
    h1,
    h2,
    tz,
    yf,
    ro,
    om,
    orr,
    load_s,
    sent,
    tin_r,
    vin_r,
    zd_r,
    zx_r,
    xc_r,
    to_r,
):
    gx = lax.axis_index("gx")
    gy = lax.axis_index("gy")
    gz = lax.axis_index("gz")
    axis = ("gy", "gx")
    pos = (gy, gx)
    half = [p // 2 for p in pos]
    core = [lax.rem(p, 2) for p in pos]
    far = [1 - h for h in half]
    near = [[f * 2 + k, f * 2 + 1 - k, h * 2 + 1 - k] for f, h, k in zip(far, half, core)]
    side_at = (
        ({"gx": lax.rem(gx + 3, 4)}, {"gx": lax.rem(gx + 1, 4)}),
        ({"gy": lax.rem(gy + 3, 4)}, {"gy": lax.rem(gy + 1, 4)}),
    )
    z_to = [lax.rem(gz + 7, 8), lax.rem(gz + 1, 8)]
    z_at = [{"gz": z_to[0]}, {"gz": z_to[1]}]
    z_near = [[pos[r]] + near[r] for r in range(2)]

    def copy(src, dst, send, recv, device):
        return pltpu.make_async_remote_copy(
            src_ref=src, dst_ref=dst, send_sem=send, recv_sem=recv, device_id=device, device_id_type=MESH
        )

    barrier = pltpu.get_barrier_semaphore()
    friends = [{axis[r]: n} for r in range(2) for n in near[r]]
    friends += z_at
    friends += [{axis[r]: n, "gz": z} for r in range(2) for n in near[r] for z in z_to]
    for device in friends:
        pl.semaphore_signal(barrier, inc=1, device_id=device, device_id_type=MESH)

    loads = [
        pltpu.make_async_copy(orb_hbm.at[:, 0], orb.at[0], load_s.at[0]),
        pltpu.make_async_copy(orb_hbm.at[:, 1], orb.at[1], load_s.at[1]),
        pltpu.make_async_copy(pot_hbm, pot, load_s.at[2]),
        pltpu.make_async_copy(mz_hbm, mz, load_s.at[3]),
        pltpu.make_async_copy(my1_hbm, my1, load_s.at[4]),
        pltpu.make_async_copy(my2_hbm, my2, load_s.at[5]),
    ]
    for one in loads:
        one.start()

    low_half = lax.broadcasted_iota(jnp.int32, (8, 128), 0) < 4
    lane8 = lax.broadcasted_iota(jnp.int32, (8, 128), 1)
    lane = lax.broadcasted_iota(jnp.int32, (48, 128), 1)

    def turn(a):
        return pltpu.roll(a, 4, 0)

    def pair(a, b):
        return jnp.where(low_half, a, turn(b)), jnp.where(low_half, turn(a), b)

    def lanes(a, by):
        return a if by % 128 == 0 else pltpu.roll(a, by % 128, 1)

    orb_rows = orb.reshape(2304, 128)
    out_rows = out.reshape(2304, 128)
    def start(c):
        c.start()

    def arrived(ref, sem):
        copy(ref, ref, sem, sem, {"gx": gx}).wait_recv()

    def tin(c, rel):
        r = c // 2
        peer = near[r][rel]
        to = {axis[r]: peer}
        return [
            copy(sm.at[c, peer], v.at[c, 0, :, pos[r]], sent.at[0], tin_r.at[c, 0], to),
            copy(sr.at[c, peer], rr.at[c, pos[r]], sent.at[1], tin_r.at[c, 1], to),
        ]

    def vin(r, rel):
        to = {axis[r]: near[r][rel]}
        return [
            copy(spm.at[r], vp.at[r, :, pos[r]], sent.at[2], vin_r.at[r, rel, 0], to),
            copy(spr.at[r], rp.at[r, pos[r]], sent.at[3], vin_r.at[r, rel, 1], to),
        ]

    def vpass():
        other, to = near[0][0], {"gy": near[0][2]}
        return [
            copy(vp.at[0, :, other], vp.at[0, :, other], sent.at[2], vin_r.at[0, 1, 0], to),
            copy(rp.at[0, other], rp.at[0, other], sent.at[3], vin_r.at[0, 1, 1], to),
        ]

    def zin(c, k, side):
        r = c // 2
        return copy(
            sz.at[c, z_near[r][k], side],
            zd.at[c, 1 - side, pos[r]],
            sent.at[4],
            zd_r.at[c],
            {axis[r]: z_near[r][k], "gz": z_to[side]},
        )

    def prepare_potential(r):
        def rows(i, start, count):
            if r == 0:
                return pot[i, start : start + count]
            return jnp.concatenate([pot[start + k, i : i + 1] for k in range(count)], axis=0)

        for i in range(12):
            spm[r, i] = rows(i, 0, 8)
        for p in range(6):
            spr[r, p] = jnp.concatenate([rows(2 * p, 8, 4), rows(2 * p + 1, 8, 4)], axis=0)
        vp[r, :, pos[r]] = spm[r]
        rp[r, pos[r]] = spr[r]

    def send_potential(r):
        for rel in ((0, 2), (1, 2, 0))[r]:
            for one in vin(r, rel):
                start(one)

    def pass_potential():
        for rel in (0, 2):
            for one in vin(0, rel):
                one.wait_recv()
        for one in vpass():
            start(one)

    def finish_potential(r):
        for one in vpass() if r == 0 else vin(1, 0) + vin(1, 1) + vin(1, 2):
            one.wait_recv()

        def scaled(a):
            return (a - CENTER) * (1.0 / HALF_WIDTH) + 3.0 * XC[0]

        def place(x, t, value):
            vq[r, x, t] = scaled(value)

        assemble(rp.at[r], place)
        for x in range(12):
            vq[r, x, 0:4] = scaled(vp[r, x])

    def prepare(c):
        def band(g, carry):
            edge = [None] * 2
            for x in range(12):
                val = orb_rows[picked(c, g, x, False), :]
                sm[c, g, x] = val
                for side in range(2):
                    r = lanes(val, 6 * x + 6 * side)
                    edge[side] = r if x == 0 else jnp.where(lane8 >= 6 * x, r, edge[side])
            for p in range(6):
                lo = orb_rows[picked(c, g, 2 * p, True), :]
                hi = orb_rows[picked(c, g, 2 * p + 1, True), :]
                val = jnp.concatenate([lo, hi], axis=0)
                sr[c, g, p] = val
                for side in range(2):
                    r = lanes(val, 72 + 6 * p + 6 * side)
                    edge[side] = jnp.where(lane8 >= 72 + 6 * p, r, edge[side])
            for side in range(2):
                sz[c, g, side] = edge[side]
            return carry

        lax.fori_loop(0, 4, band, 0)

    def send_in(c):
        for k in (1, 2, 0, 3):
            for side in range(2):
                start(zin(c, k, side))
        for rel in range(3):
            for one in tin(c, rel):
                start(one)
        me = pos[c // 2]
        v[c, 0, :, me] = sm[c, me]
        rr[c, me] = sr[c, me]

    def assemble(rest, dest):
        for p in range(6):
            for t in range(2):
                even, odd = pair(rest[2 * t, p], rest[2 * t + 1, p])
                dest(2 * p, 4 + t, even)
                dest(2 * p + 1, 4 + t, odd)

    def zx(c, side):
        return copy(zs.at[c, side], zr.at[c, 1 - side], sent.at[5], zx_r.at[c, side], z_at[side])

    def edges(c):
        low = None
        high = None
        for x in range(12):
            val = v[c, 1, x].reshape(48, 128)
            a = lanes(val, 6 * x)
            b = lanes(val, 6 * x + 6)
            low = a if x == 0 else jnp.where(lane >= 6 * x, a, low)
            high = b if x == 0 else jnp.where(lane >= 6 * x, b, high)
        zs[c, 0] = low.reshape(6, 8, 128)
        zs[c, 1] = high.reshape(6, 8, 128)
        for side in range(2):
            start(zx(c, side))

    def stage_a(c):
        arrived(v.at[c, 0, :, 0:3], tin_r.at[c, 0])
        arrived(rr.at[c, 0:3], tin_r.at[c, 1])

        def dest(x, t, value):
            v[c, 0, x, t] = value

        assemble(rr.at[c], dest)

    def xc(c, step, side, piece):
        return copy(
            cs.at[c, step, piece, side],
            cr.at[c, step, piece, side],
            sent.at[6],
            xc_r.at[c, step, piece],
            side_at[c // 2][side],
        )

    def halo(c, step):
        if step == 1:
            for side in range(2):
                zx(c, side).wait_recv()
            far_side = [zr[c, side].reshape(48, 128) for side in range(2)]
            return lambda side, x, by: lanes(far_side[side], by - 6 * x)
        arrived(zd.at[c], zd_r.at[c])
        main = []
        rest = []
        for side in range(2):
            tiles = [zd[c, side, s] for s in range(4)]
            main.append(jnp.concatenate(tiles, axis=0))
            both = [pair(tiles[2 * t], tiles[2 * t + 1]) for t in range(2)]
            rest.append([jnp.concatenate([both[0][k], both[1][k]], axis=0) for k in range(2)])

        def edge(side, x, by):
            a = lanes(main[side], by - 6 * x)
            b = lanes(rest[side][x % 2], by - 72 - 6 * (x // 2))
            return jnp.concatenate([a, b], axis=0)

        return edge

    def block_of(c, piece):
        return far[c // 2] if piece == 0 else half[c // 2]

    def piece_tile(c, piece, i):
        block = block_of(c, piece)
        return 2 * block + i if i < 2 else 4 + block

    def stage_b(c, step):
        for x in range(12):
            a, b = split(v[c, step, x].reshape(48, 128))
            v1[x] = a
            v2[x] = b
        for xp in range(6):
            x0, x1 = 2 * xp, 2 * xp + 1
            a = jnp.concatenate([v1[x0], v1[x1]], axis=1)
            b = jnp.concatenate([v2[x0], v2[x1]], axis=1)
            q = jnp.dot(my1[c // 2], jnp.concatenate([a, b, a], axis=0), preferred_element_type=F32)
            for i, x in enumerate((x0, x1)):
                wf[x] = q[0:48, 128 * i : 128 * i + 128].reshape(6, 8, 128)
                part[c, x] = q[48:96, 128 * i : 128 * i + 128].reshape(6, 8, 128)
        edge = halo(c, step)
        for x in range(12):
            up = edge(1, x, 128)
            down = edge(0, x, 122)
            h = jnp.where(lane < 6, up, jnp.where(lane >= 122, down, 0.0))
            a, b = split(h)
            h1[x] = a
            h2[x] = b
        for part_rows in range(2):
            xs = slice(6 * part_rows, 6 * part_rows + 6)
            f1 = v1[xs].reshape(288, 128)
            f2 = v2[xs].reshape(288, 128)
            g1 = h1[xs].reshape(288, 128)
            g2 = h2[xs].reshape(288, 128)
            acc = jnp.dot(jnp.concatenate([f1, f2], axis=1), mz[0], preferred_element_type=F32)
            acc += jnp.dot(jnp.concatenate([f1, g1], axis=1), mz[1], preferred_element_type=F32)
            acc += jnp.dot(jnp.concatenate([g1, g2], axis=1), mz[2], preferred_element_type=F32)
            tz[288 * part_rows : 288 * part_rows + 288] = acc
        for xp in range(6):
            x0, x1 = 2 * xp, 2 * xp + 1
            t = jnp.concatenate([tz[48 * x0 : 48 * x0 + 48, 0:128], tz[48 * x1 : 48 * x1 + 48, 0:128]], axis=1)
            s = jnp.concatenate([tz[48 * x0 : 48 * x0 + 48, 128:256], tz[48 * x1 : 48 * x1 + 48, 128:256]], axis=1)
            ta, tb = split(t)
            r = jnp.dot(my2[c // 2], jnp.concatenate([ta, tb, ta], axis=0), preferred_element_type=F32)
            r = r + s
            for i, x in enumerate((x0, x1)):
                wf[x] = wf[x] + t[:, 128 * i : 128 * i + 128].reshape(6, 8, 128)
                part[c, x] = part[c, x] + r[:, 128 * i : 128 * i + 128].reshape(6, 8, 128)

        for piece in range(2):
            block = block_of(c, piece)

            def tile(i, carry):
                t = (i // 2) * (4 + block) + (1 - i // 2) * (2 * block + i)
                acc = [None] * 24
                for j in range(12):
                    vj = v[c, step, j, t]
                    wj = wf[j, t]
                    for k in range(1, 7):
                        cv = XC[k] * vj
                        aw = XA[c // 2][k - 1] * wj
                        lo, hi = j + 6 - k, j + 6 + k
                        acc[lo] = cv + aw if acc[lo] is None else acc[lo] + (cv + aw)
                        acc[hi] = cv - aw if acc[hi] is None else acc[hi] + (cv - aw)
                for j in range(6):
                    cs[c, step, piece, 0, j, i] = acc[j]
                    cs[c, step, piece, 1, j, i] = acc[18 + j]
                for j in range(12):
                    part[c, j, t] = part[c, j, t] + acc[6 + j]
                return carry

            lax.fori_loop(0, 3, tile, 0, unroll=True)
            for side in range(2):
                start(xc(c, step, side, piece))

    def to(c, rel):
        r = c // 2
        peer = near[r][rel]
        at = {axis[r]: peer}
        return [
            copy(yf.at[c, :, peer], om.at[c, pos[r]], sent.at[7], to_r.at[c, 0], at),
            copy(ro.at[c, peer], orr.at[c, pos[r]], sent.at[8], to_r.at[c, 1], at),
        ]

    def stage_c(c, step):
        for piece in range(2):
            arrived(cr.at[c, step, piece], xc_r.at[c, step, piece])
            for i in range(3):
                t = piece_tile(c, piece, i)
                got = jnp.concatenate([cr[c, step, piece, 1, :, i], cr[c, step, piece, 0, :, i]], axis=0)
                y = part[c, :, t] + got + vq[c // 2, :, t] * v[c, step, :, t]
                if step == 0:
                    v[c, 1, :, t] = y
                else:
                    yf[c, :, t] = 2.0 * y - v[c, 0, :, t]
            if step == 0:
                continue
            block = block_of(c, piece)
            for p in range(6):
                even, odd = pair(yf[c, 2 * p, 4 + block], yf[c, 2 * p + 1, 4 + block])
                ro[c, 2 * block, p] = even
                ro[c, 2 * block + 1, p] = odd
            for rel in (0, 1) if piece == 0 else (2,):
                for one in to(c, rel):
                    start(one)
        if step == 0:
            edges(c)
            return
        me = pos[c // 2]
        om[c, me] = yf[c, :, me]
        orr[c, me] = ro[c, me]

    def stage_d(c):
        arrived(om.at[c, 0:3], to_r.at[c, 0])
        arrived(orr.at[c, 0:3], to_r.at[c, 1])

        def band(g, carry):
            for x in range(12):
                out_rows[picked(c, g, x, False), :] = om[c, g, x]
            for p in range(6):
                r = orr[c, g, p]
                out_rows[picked(c, g, 2 * p, True), :] = r[0:4]
                out_rows[picked(c, g, 2 * p + 1, True), :] = r[4:8]
            return carry

        lax.fori_loop(0, 4, band, 0)

    loads[0].wait()
    prepare(0)
    loads[1].wait()
    pl.semaphore_wait(barrier, len(friends))
    send_in(0)
    for c in (2, 1, 3):
        prepare(c)
        send_in(c)
    loads[2].wait()
    prepare_potential(0)
    send_potential(0)
    prepare_potential(1)
    for one in loads[3:]:
        one.wait()

    send_potential(1)
    stage_a(0)
    stage_b(0, 0)
    stage_a(2)
    stage_b(2, 0)
    stage_a(1)
    stage_b(1, 0)
    pass_potential()
    stage_a(3)
    stage_b(3, 0)
    finish_potential(0)
    finish_potential(1)
    stage_c(2, 0)
    stage_c(0, 0)
    stage_c(3, 0)
    stage_b(2, 1)
    stage_c(1, 0)
    stage_b(0, 1)
    stage_b(3, 1)
    stage_b(1, 1)
    stage_c(2, 1)
    stage_c(0, 1)
    stage_c(3, 1)
    stage_c(1, 1)
    for c in (2, 0, 3, 1):
        stage_d(c)
    done = [sm.at[:, 0:3], sr.at[:, 0:3], vp.at[:, :, 0:3], rp.at[:, 0:3], sz, zs, cs, yf.at[:, :, 0:3], ro.at[:, 0:3]]
    for i, ref in enumerate(done):
        copy(ref, ref, sent.at[i], sent.at[i], {"gx": gx}).wait_send()


def place_kernel(out, out_hbm, store_s):
    stores = [
        pltpu.make_async_copy(out.at[h, 36 * k : 36 * k + 36], out_hbm.at[36 * k : 36 * k + 36, h], store_s.at[h, k])
        for h in range(2)
        for k in range(4)
    ]
    for one in stores:
        one.start()
    for one in stores:
        one.wait()


def local(orbitals, potential):
    rows = jnp.transpose(orbitals, (1, 2, 0, 3)).reshape(144, 2, 8, 128)
    pairs = [y_matrices(G02, G12), y_matrices(G12, G02)]
    my1, my2 = (np.stack([p[i] for p in pairs]) for i in range(2))
    hbm = pl.BlockSpec(memory_space=pltpu.HBM)
    chip = pl.BlockSpec(memory_space=pltpu.VMEM)
    tile = (6, 8, 128)
    slab = (12, *tile)
    sem = pltpu.SemaphoreType.DMA

    def vmem(*shape, dtype=F32):
        return pltpu.VMEM(shape, dtype)

    inputs = [rows, potential, jnp.asarray(z_matrices()), jnp.asarray(my1), jnp.asarray(my2)]
    inputs = [pltpu.with_memory_space_constraint(a, pltpu.HBM) for a in inputs]
    placed = pl.pallas_call(
        kernel,
        out_shape=jax.ShapeDtypeStruct((2, 144, 8, 128), F32),
        in_specs=[hbm] * 5,
        out_specs=chip,
        scratch_shapes=[
            vmem(2, 144, 8, 128),
            vmem(12, 12, 128),
            vmem(3, 256, 256, dtype=BF16),
            vmem(2, 96, 144, dtype=BF16),
            vmem(2, 48, 144, dtype=BF16),
            vmem(4, 4, 12, 8, 128),
            vmem(4, 4, *tile),
            vmem(4, 4, 2, 8, 128),
            vmem(2, 12, 8, 128),
            vmem(2, *tile),
            vmem(4, 2, *slab),
            vmem(4, 4, *tile),
            vmem(2, 12, 4, 8, 128),
            vmem(2, *slab),
            vmem(2, 4, *tile),
            vmem(4, 2, 4, 8, 128),
            vmem(4, 2, *tile),
            vmem(4, 2, *tile),
            vmem(4, 2, 2, 2, 6, 3, 8, 128),
            vmem(4, 2, 2, 2, 6, 3, 8, 128),
            vmem(4, *slab),
            vmem(*slab),
            vmem(12, 48, 128, dtype=BF16),
            vmem(12, 48, 128, dtype=BF16),
            vmem(12, 48, 128, dtype=BF16),
            vmem(12, 48, 128, dtype=BF16),
            vmem(576, 256),
            vmem(4, *slab),
            vmem(4, 4, *tile),
            vmem(4, 4, 12, 8, 128),
            vmem(4, 4, *tile),
            sem((8,)),
            sem((9,)),
            sem((4, 2)),
            sem((2, 3, 2)),
            sem((4,)),
            sem((4, 2)),
            sem((4, 2, 2)),
            sem((4, 2)),
        ],
        compiler_params=pltpu.CompilerParams(
            collective_id=0, has_side_effects=True, vmem_limit_bytes=24 * 1024 * 1024
        ),
    )(*inputs)
    out = pl.pallas_call(
        place_kernel,
        out_shape=jax.ShapeDtypeStruct((144, 2, 8, 128), F32),
        in_specs=[chip],
        out_specs=hbm,
        scratch_shapes=[sem((2, 4))],
        compiler_params=pltpu.CompilerParams(vmem_limit_bytes=8 * 1024 * 1024),
    )(placed)
    return jnp.transpose(out.reshape(12, 12, 16, 128), (2, 0, 1, 3))


def solution(mesh):
    return jax.shard_map(
        local,
        mesh=mesh,
        in_specs=(P(None, "gx", "gy", "gz"), P("gx", "gy", "gz")),
        out_specs=P(None, "gx", "gy", "gz"),
        check_vma=False,
    )
```

```python
import functools

import jax
import jax.numpy as jnp
import numpy as np
from jax import lax
from jax.experimental import pallas as pl
from jax.experimental.pallas import tpu as pltpu
from jax.sharding import PartitionSpec as P

MESH = pl.DeviceIdType.MESH
SECOND = (
    -5369.0 / 1800.0,
    12.0 / 7.0,
    -15.0 / 56.0,
    10.0 / 189.0,
    -1.0 / 112.0,
    2.0 / 1925.0,
    -1.0 / 16632.0,
)
FIRST = (6.0 / 7.0, -15.0 / 56.0, 5.0 / 63.0, -1.0 / 56.0, 3.0 / 385.0, -1.0 / 792.0)
G01, G02, G12 = 0.25, 0.15, 0.2
CENTER = 10.5
HALF_WIDTH = 9.5
SIGMA = -0.5 / HALF_WIDTH

XC = [SIGMA * c for c in SECOND]
XA = [[SIGMA * 2.0 * g * a for a in FIRST] for g in (G02, G12)]

F32 = jnp.float32
BF16 = jnp.bfloat16


def order_of_rows():
    rows = []
    for s in range(4):
        rows += [12 * s + r for r in range(8)]
    for s in range(4):
        rows += [12 * s + 8 + r for r in range(4)]
    return rows


def two_parts(m):
    hi = m.astype(np.float32).astype(jnp.bfloat16)
    lo = (m - hi.astype(np.float64)).astype(np.float32).astype(jnp.bfloat16)
    return hi, lo


def z_matrices():
    m = np.zeros((140, 256))
    for z in range(128):
        for k in range(1, 7):
            m[z + 6 + k, z] += FIRST[k - 1]
            m[z + 6 - k, z] -= FIRST[k - 1]
            m[z + 6 + k, 128 + z] += SIGMA * SECOND[k]
            m[z + 6 - k, 128 + z] += SIGMA * SECOND[k]
    inside = m[6:134]
    halo = np.zeros((128, 256))
    halo[122:128] = m[0:6]
    halo[0:6] = m[134:140]
    i1, i2 = two_parts(inside)
    h1, h2 = two_parts(halo)
    return np.stack([np.concatenate([i1, i1]), np.concatenate([i2, h1]), np.concatenate([h2, h1])])


def y_matrices(g_here, g_other):
    rows = order_of_rows()
    place = {y: r for r, y in enumerate(rows)}
    d1 = np.zeros((48, 48))
    d2 = np.zeros((48, 48))
    for y in range(48):
        for k in range(1, 7):
            d1[place[y], place[(y + k) % 48]] += FIRST[k - 1]
            d1[place[y], place[(y - k) % 48]] -= FIRST[k - 1]
            d2[place[y], place[(y + k) % 48]] += SECOND[k]
            d2[place[y], place[(y - k) % 48]] += SECOND[k]
    a1, a2 = two_parts(np.concatenate([(G01 / g_here) * d1, SIGMA * d2]))
    b1, b2 = two_parts(SIGMA * 2.0 * g_other * d1)
    return np.concatenate([a1, a1, a2], axis=1), np.concatenate([b1, b1, b2], axis=1)


def split(value):
    hi = value.astype(BF16)
    lo = (value - hi.astype(F32)).astype(BF16)
    return hi, lo


def picked(c, g, i, rest):
    if c < 2:
        first, step = i * 96, 8
    else:
        first, step = 1152 + i * 8, 96
    first = first + 4 * (c % 2) + g
    return pl.ds(first + 8 * step, 4, stride=step) if rest else pl.ds(first, 8, stride=step)


def kernel(
    orb_hbm,
    pot_hbm,
    mz_hbm,
    my1_hbm,
    my2_hbm,
    out,
    orb,
    pot,
    mz,
    my1,
    my2,
    sm,
    sr,
    sz,
    spm,
    spr,
    v,
    rr,
    vp,
    vq,
    rp,
    zd,
    zs,
    zr,
    cs,
    cr,
    part,
    wf,
    v1,
    v2,
    h1,
    h2,
    tz,
    yf,
    ro,
    om,
    orr,
    load_s,
    sent,
    tin_r,
    vin_r,
    zd_r,
    zx_r,
    xc_r,
    to_r,
):
    gx = lax.axis_index("gx")
    gy = lax.axis_index("gy")
    gz = lax.axis_index("gz")
    axis = ("gy", "gx")
    pos = (gy, gx)
    half = [p // 2 for p in pos]
    core = [lax.rem(p, 2) for p in pos]
    far = [1 - h for h in half]
    near = [[f * 2 + k, f * 2 + 1 - k, h * 2 + 1 - k] for f, h, k in zip(far, half, core)]
    side_at = (
        ({"gx": lax.rem(gx + 3, 4)}, {"gx": lax.rem(gx + 1, 4)}),
        ({"gy": lax.rem(gy + 3, 4)}, {"gy": lax.rem(gy + 1, 4)}),
    )
    z_to = [lax.rem(gz + 7, 8), lax.rem(gz + 1, 8)]
    z_at = [{"gz": z_to[0]}, {"gz": z_to[1]}]
    z_near = [[pos[r]] + near[r] for r in range(2)]

    def copy(src, dst, send, recv, device):
        return pltpu.make_async_remote_copy(
            src_ref=src, dst_ref=dst, send_sem=send, recv_sem=recv, device_id=device, device_id_type=MESH
        )

    barrier = pltpu.get_barrier_semaphore()
    friends = [{axis[r]: n} for r in range(2) for n in near[r]]
    friends += z_at
    friends += [{axis[r]: n, "gz": z} for r in range(2) for n in near[r] for z in z_to]
    for device in friends:
        pl.semaphore_signal(barrier, inc=1, device_id=device, device_id_type=MESH)

    loads = [
        pltpu.make_async_copy(orb_hbm.at[:, 0], orb.at[0], load_s.at[0]),
        pltpu.make_async_copy(orb_hbm.at[:, 1], orb.at[1], load_s.at[1]),
        pltpu.make_async_copy(pot_hbm, pot, load_s.at[2]),
        pltpu.make_async_copy(mz_hbm, mz, load_s.at[3]),
        pltpu.make_async_copy(my1_hbm, my1, load_s.at[4]),
        pltpu.make_async_copy(my2_hbm, my2, load_s.at[5]),
    ]
    for one in loads:
        one.start()

    low_half = lax.broadcasted_iota(jnp.int32, (8, 128), 0) < 4
    lane8 = lax.broadcasted_iota(jnp.int32, (8, 128), 1)
    lane = lax.broadcasted_iota(jnp.int32, (48, 128), 1)

    def turn(a):
        return pltpu.roll(a, 4, 0)

    def pair(a, b):
        return jnp.where(low_half, a, turn(b)), jnp.where(low_half, turn(a), b)

    def lanes(a, by):
        return a if by % 128 == 0 else pltpu.roll(a, by % 128, 1)

    orb_rows = orb.reshape(2304, 128)
    out_rows = out.reshape(2304, 128)
    def start(c):
        c.start()

    def arrived(ref, sem):
        copy(ref, ref, sem, sem, {"gx": gx}).wait_recv()

    def tin(c, rel):
        r = c // 2
        peer = near[r][rel]
        to = {axis[r]: peer}
        return [
            copy(sm.at[c, peer], v.at[c, 0, :, pos[r]], sent.at[0], tin_r.at[c, 0], to),
            copy(sr.at[c, peer], rr.at[c, pos[r]], sent.at[1], tin_r.at[c, 1], to),
        ]

    def vin(r, rel):
        to = {axis[r]: near[r][rel]}
        return [
            copy(spm.at[r], vp.at[r, :, pos[r]], sent.at[2], vin_r.at[r, rel, 0], to),
            copy(spr.at[r], rp.at[r, pos[r]], sent.at[3], vin_r.at[r, rel, 1], to),
        ]

    def vpass():
        other, to = near[0][0], {"gy": near[0][2]}
        return [
            copy(vp.at[0, :, other], vp.at[0, :, other], sent.at[2], vin_r.at[0, 1, 0], to),
            copy(rp.at[0, other], rp.at[0, other], sent.at[3], vin_r.at[0, 1, 1], to),
        ]

    def zin(c, k, side):
        r = c // 2
        return copy(
            sz.at[c, z_near[r][k], side],
            zd.at[c, 1 - side, pos[r]],
            sent.at[4],
            zd_r.at[c],
            {axis[r]: z_near[r][k], "gz": z_to[side]},
        )

    def prepare_potential(r):
        def rows(i, start, count):
            if r == 0:
                return pot[i, start : start + count]
            return jnp.concatenate([pot[start + k, i : i + 1] for k in range(count)], axis=0)

        for i in range(12):
            spm[r, i] = rows(i, 0, 8)
        for p in range(6):
            spr[r, p] = jnp.concatenate([rows(2 * p, 8, 4), rows(2 * p + 1, 8, 4)], axis=0)
        vp[r, :, pos[r]] = spm[r]
        rp[r, pos[r]] = spr[r]

    def send_potential(r):
        for rel in ((0, 2), (1, 2, 0))[r]:
            for one in vin(r, rel):
                start(one)

    def pass_potential():
        for rel in (0, 2):
            for one in vin(0, rel):
                one.wait_recv()
        for one in vpass():
            start(one)

    def finish_potential(r):
        for one in vpass() if r == 0 else vin(1, 0) + vin(1, 1) + vin(1, 2):
            one.wait_recv()

        def scaled(a):
            return (a - CENTER) * (1.0 / HALF_WIDTH) + 3.0 * XC[0]

        def place(x, t, value):
            vq[r, x, t] = scaled(value)

        assemble(rp.at[r], place)
        for x in range(12):
            vq[r, x, 0:4] = scaled(vp[r, x])

    def prepare(c):
        def band(g, carry):
            edge = [None] * 2
            for x in range(12):
                val = orb_rows[picked(c, g, x, False), :]
                sm[c, g, x] = val
                for side in range(2):
                    r = lanes(val, 6 * x + 6 * side)
                    edge[side] = r if x == 0 else jnp.where(lane8 >= 6 * x, r, edge[side])
            for p in range(6):
                lo = orb_rows[picked(c, g, 2 * p, True), :]
                hi = orb_rows[picked(c, g, 2 * p + 1, True), :]
                val = jnp.concatenate([lo, hi], axis=0)
                sr[c, g, p] = val
                for side in range(2):
                    r = lanes(val, 72 + 6 * p + 6 * side)
                    edge[side] = jnp.where(lane8 >= 72 + 6 * p, r, edge[side])
            for side in range(2):
                sz[c, g, side] = edge[side]
            return carry

        lax.fori_loop(0, 4, band, 0)

    def send_in(c):
        for k in (1, 2, 0, 3):
            for side in range(2):
                start(zin(c, k, side))
        for rel in range(3):
            for one in tin(c, rel):
                start(one)
        me = pos[c // 2]
        v[c, 0, :, me] = sm[c, me]
        rr[c, me] = sr[c, me]

    def assemble(rest, dest):
        for p in range(6):
            for t in range(2):
                even, odd = pair(rest[2 * t, p], rest[2 * t + 1, p])
                dest(2 * p, 4 + t, even)
                dest(2 * p + 1, 4 + t, odd)

    def zx(c, side):
        return copy(zs.at[c, side], zr.at[c, 1 - side], sent.at[5], zx_r.at[c, side], z_at[side])

    def edges(c):
        low = None
        high = None
        for x in range(12):
            val = v[c, 1, x].reshape(48, 128)
            a = lanes(val, 6 * x)
            b = lanes(val, 6 * x + 6)
            low = a if x == 0 else jnp.where(lane >= 6 * x, a, low)
            high = b if x == 0 else jnp.where(lane >= 6 * x, b, high)
        zs[c, 0] = low.reshape(6, 8, 128)
        zs[c, 1] = high.reshape(6, 8, 128)
        for side in range(2):
            start(zx(c, side))

    def stage_a(c):
        arrived(v.at[c, 0, :, 0:3], tin_r.at[c, 0])
        arrived(rr.at[c, 0:3], tin_r.at[c, 1])

        def dest(x, t, value):
            v[c, 0, x, t] = value

        assemble(rr.at[c], dest)

    def xc(c, step, side, piece):
        return copy(
            cs.at[c, step, piece, side],
            cr.at[c, step, piece, side],
            sent.at[6],
            xc_r.at[c, step, piece],
            side_at[c // 2][side],
        )

    def halo(c, step):
        if step == 1:
            for side in range(2):
                zx(c, side).wait_recv()
            far_side = [zr[c, side].reshape(48, 128) for side in range(2)]
            return lambda side, x, by: lanes(far_side[side], by - 6 * x)
        arrived(zd.at[c], zd_r.at[c])
        main = []
        rest = []
        for side in range(2):
            tiles = [zd[c, side, s] for s in range(4)]
            main.append(jnp.concatenate(tiles, axis=0))
            both = [pair(tiles[2 * t], tiles[2 * t + 1]) for t in range(2)]
            rest.append([jnp.concatenate([both[0][k], both[1][k]], axis=0) for k in range(2)])

        def edge(side, x, by):
            a = lanes(main[side], by - 6 * x)
            b = lanes(rest[side][x % 2], by - 72 - 6 * (x // 2))
            return jnp.concatenate([a, b], axis=0)

        return edge

    def block_of(c, piece):
        return far[c // 2] if piece == 0 else half[c // 2]

    def piece_tile(c, piece, i):
        block = block_of(c, piece)
        return 2 * block + i if i < 2 else 4 + block

    def stage_b(c, step):
        for x in range(12):
            a, b = split(v[c, step, x].reshape(48, 128))
            v1[x] = a
            v2[x] = b
        edge = halo(c, step)
        for x in range(12):
            up = edge(1, x, 128)
            down = edge(0, x, 122)
            h = jnp.where(lane < 6, up, jnp.where(lane >= 122, down, 0.0))
            a, b = split(h)
            h1[x] = a
            h2[x] = b
        for part_rows in range(2):
            xs = slice(6 * part_rows, 6 * part_rows + 6)
            f1 = v1[xs].reshape(288, 128)
            f2 = v2[xs].reshape(288, 128)
            g1 = h1[xs].reshape(288, 128)
            g2 = h2[xs].reshape(288, 128)
            acc = jnp.dot(jnp.concatenate([f1, f2], axis=1), mz[0], preferred_element_type=F32)
            acc += jnp.dot(jnp.concatenate([f1, g1], axis=1), mz[1], preferred_element_type=F32)
            acc += jnp.dot(jnp.concatenate([g1, g2], axis=1), mz[2], preferred_element_type=F32)
            tz[288 * part_rows : 288 * part_rows + 288] = acc
        for xp in range(6):
            x0, x1 = 2 * xp, 2 * xp + 1
            a = jnp.concatenate([v1[x0], v1[x1]], axis=1)
            b = jnp.concatenate([v2[x0], v2[x1]], axis=1)
            q = jnp.dot(my1[c // 2], jnp.concatenate([a, b, a], axis=0), preferred_element_type=F32)
            t = jnp.concatenate([tz[48 * x0 : 48 * x0 + 48, 0:128], tz[48 * x1 : 48 * x1 + 48, 0:128]], axis=1)
            s = jnp.concatenate([tz[48 * x0 : 48 * x0 + 48, 128:256], tz[48 * x1 : 48 * x1 + 48, 128:256]], axis=1)
            ta, tb = split(t)
            r = jnp.dot(my2[c // 2], jnp.concatenate([ta, tb, ta], axis=0), preferred_element_type=F32)
            w = q[0:48] + t
            r = r + q[48:96] + s
            for i, x in enumerate((x0, x1)):
                wf[x] = w[:, 128 * i : 128 * i + 128].reshape(6, 8, 128)
                part[c, x] = r[:, 128 * i : 128 * i + 128].reshape(6, 8, 128)

        for piece in range(2):
            block = block_of(c, piece)

            def tile(i, carry):
                t = (i // 2) * (4 + block) + (1 - i // 2) * (2 * block + i)
                acc = [None] * 24
                for j in range(12):
                    vj = v[c, step, j, t]
                    wj = wf[j, t]
                    for k in range(1, 7):
                        cv = XC[k] * vj
                        aw = XA[c // 2][k - 1] * wj
                        lo, hi = j + 6 - k, j + 6 + k
                        acc[lo] = cv + aw if acc[lo] is None else acc[lo] + (cv + aw)
                        acc[hi] = cv - aw if acc[hi] is None else acc[hi] + (cv - aw)
                for j in range(6):
                    cs[c, step, piece, 0, j, i] = acc[j]
                    cs[c, step, piece, 1, j, i] = acc[18 + j]
                for j in range(12):
                    part[c, j, t] = part[c, j, t] + acc[6 + j]
                return carry

            lax.fori_loop(0, 3, tile, 0, unroll=True)
            for side in range(2):
                start(xc(c, step, side, piece))

    def to(c, rel):
        r = c // 2
        peer = near[r][rel]
        at = {axis[r]: peer}
        return [
            copy(yf.at[c, :, peer], om.at[c, pos[r]], sent.at[7], to_r.at[c, 0], at),
            copy(ro.at[c, peer], orr.at[c, pos[r]], sent.at[8], to_r.at[c, 1], at),
        ]

    def stage_c(c, step):
        for piece in range(2):
            arrived(cr.at[c, step, piece], xc_r.at[c, step, piece])
            for i in range(3):
                t = piece_tile(c, piece, i)
                got = jnp.concatenate([cr[c, step, piece, 1, :, i], cr[c, step, piece, 0, :, i]], axis=0)
                y = part[c, :, t] + got + vq[c // 2, :, t] * v[c, step, :, t]
                if step == 0:
                    v[c, 1, :, t] = y
                else:
                    yf[c, :, t] = 2.0 * y - v[c, 0, :, t]
            if step == 0:
                continue
            block = block_of(c, piece)
            for p in range(6):
                even, odd = pair(yf[c, 2 * p, 4 + block], yf[c, 2 * p + 1, 4 + block])
                ro[c, 2 * block, p] = even
                ro[c, 2 * block + 1, p] = odd
            for rel in (0, 1) if piece == 0 else (2,):
                for one in to(c, rel):
                    start(one)
        if step == 0:
            edges(c)
            return
        me = pos[c // 2]
        om[c, me] = yf[c, :, me]
        orr[c, me] = ro[c, me]

    def stage_d(c):
        arrived(om.at[c, 0:3], to_r.at[c, 0])
        arrived(orr.at[c, 0:3], to_r.at[c, 1])

        def band(g, carry):
            for x in range(12):
                out_rows[picked(c, g, x, False), :] = om[c, g, x]
            for p in range(6):
                r = orr[c, g, p]
                out_rows[picked(c, g, 2 * p, True), :] = r[0:4]
                out_rows[picked(c, g, 2 * p + 1, True), :] = r[4:8]
            return carry

        lax.fori_loop(0, 4, band, 0)

    loads[0].wait()
    prepare(0)
    loads[1].wait()
    pl.semaphore_wait(barrier, len(friends))
    send_in(0)
    for c in (2, 1, 3):
        prepare(c)
        send_in(c)
    loads[2].wait()
    prepare_potential(0)
    send_potential(0)
    prepare_potential(1)
    for one in loads[3:]:
        one.wait()

    send_potential(1)
    stage_a(2)
    stage_b(2, 0)
    stage_a(0)
    stage_b(0, 0)
    stage_a(3)
    stage_b(3, 0)
    pass_potential()
    stage_a(1)
    stage_b(1, 0)
    finish_potential(0)
    finish_potential(1)
    stage_c(2, 0)
    stage_c(0, 0)
    stage_c(3, 0)
    stage_b(2, 1)
    stage_c(1, 0)
    stage_b(0, 1)
    stage_b(3, 1)
    stage_b(1, 1)
    stage_c(2, 1)
    stage_c(0, 1)
    stage_c(3, 1)
    stage_c(1, 1)
    for c in (2, 0, 3, 1):
        stage_d(c)
    done = [sm.at[:, 0:3], sr.at[:, 0:3], vp.at[:, :, 0:3], rp.at[:, 0:3], sz, zs, cs, yf.at[:, :, 0:3], ro.at[:, 0:3]]
    for i, ref in enumerate(done):
        copy(ref, ref, sent.at[i], sent.at[i], {"gx": gx}).wait_send()


def place_kernel(out, out_hbm, store_s):
    stores = [
        pltpu.make_async_copy(out.at[h, 36 * k : 36 * k + 36], out_hbm.at[36 * k : 36 * k + 36, h], store_s.at[h, k])
        for h in range(2)
        for k in range(4)
    ]
    for one in stores:
        one.start()
    for one in stores:
        one.wait()


def local(orbitals, potential):
    rows = jnp.transpose(orbitals, (1, 2, 0, 3)).reshape(144, 2, 8, 128)
    pairs = [y_matrices(G02, G12), y_matrices(G12, G02)]
    my1, my2 = (np.stack([p[i] for p in pairs]) for i in range(2))
    hbm = pl.BlockSpec(memory_space=pltpu.HBM)
    chip = pl.BlockSpec(memory_space=pltpu.VMEM)
    tile = (6, 8, 128)
    slab = (12, *tile)
    sem = pltpu.SemaphoreType.DMA

    def vmem(*shape, dtype=F32):
        return pltpu.VMEM(shape, dtype)

    inputs = [rows, potential, jnp.asarray(z_matrices()), jnp.asarray(my1), jnp.asarray(my2)]
    inputs = [pltpu.with_memory_space_constraint(a, pltpu.HBM) for a in inputs]
    placed = pl.pallas_call(
        kernel,
        out_shape=jax.ShapeDtypeStruct((2, 144, 8, 128), F32),
        in_specs=[hbm] * 5,
        out_specs=chip,
        scratch_shapes=[
            vmem(2, 144, 8, 128),
            vmem(12, 12, 128),
            vmem(3, 256, 256, dtype=BF16),
            vmem(2, 96, 144, dtype=BF16),
            vmem(2, 48, 144, dtype=BF16),
            vmem(4, 4, 12, 8, 128),
            vmem(4, 4, *tile),
            vmem(4, 4, 2, 8, 128),
            vmem(2, 12, 8, 128),
            vmem(2, *tile),
            vmem(4, 2, *slab),
            vmem(4, 4, *tile),
            vmem(2, 12, 4, 8, 128),
            vmem(2, *slab),
            vmem(2, 4, *tile),
            vmem(4, 2, 4, 8, 128),
            vmem(4, 2, *tile),
            vmem(4, 2, *tile),
            vmem(4, 2, 2, 2, 6, 3, 8, 128),
            vmem(4, 2, 2, 2, 6, 3, 8, 128),
            vmem(4, *slab),
            vmem(*slab),
            vmem(12, 48, 128, dtype=BF16),
            vmem(12, 48, 128, dtype=BF16),
            vmem(12, 48, 128, dtype=BF16),
            vmem(12, 48, 128, dtype=BF16),
            vmem(576, 256),
            vmem(4, *slab),
            vmem(4, 4, *tile),
            vmem(4, 4, 12, 8, 128),
            vmem(4, 4, *tile),
            sem((8,)),
            sem((9,)),
            sem((4, 2)),
            sem((2, 3, 2)),
            sem((4,)),
            sem((4, 2)),
            sem((4, 2, 2)),
            sem((4, 2)),
        ],
        compiler_params=pltpu.CompilerParams(
            collective_id=0, has_side_effects=True, vmem_limit_bytes=24 * 1024 * 1024
        ),
    )(*inputs)
    out = pl.pallas_call(
        place_kernel,
        out_shape=jax.ShapeDtypeStruct((144, 2, 8, 128), F32),
        in_specs=[chip],
        out_specs=hbm,
        scratch_shapes=[sem((2, 4))],
        compiler_params=pltpu.CompilerParams(vmem_limit_bytes=8 * 1024 * 1024),
    )(placed)
    return jnp.transpose(out.reshape(12, 12, 16, 128), (2, 0, 1, 3))


def solution(mesh):
    return jax.shard_map(
        local,
        mesh=mesh,
        in_specs=(P(None, "gx", "gy", "gz"), P("gx", "gy", "gz")),
        out_specs=P(None, "gx", "gy", "gz"),
        check_vma=False,
    )
```
